16 devices in a mesh: tp: 2 (over z), fsdp: 8 (over y, x, core).
Axes of the slice: x: 2, y: 2, z: 2, core: 2. Of those that a mesh axis runs over, the one named last changes fastest.
Arguments:
- patches: bfloat16 [256, 49, 3072], P('fsdp')
- labels: int32 [256], P('fsdp')
- w_stem: float32 [3072, 512], P('fsdp', 'tp')
- b_stem: float32 [512], P(('tp', 'fsdp'))
- ln1_g: float32 [2, 512], P(None, ('tp', 'fsdp'))
- ln1_b: float32 [2, 512], P(None, ('tp', 'fsdp'))
- w_tok1: float32 [2, 49, 256], P(None, None, 'fsdp')
- b_tok1: float32 [2, 256], P(None, 'fsdp')
- w_tok2: float32 [2, 256, 49], P(None, 'fsdp')
- ln2_g: float32 [2, 512], P(None, ('tp', 'fsdp'))
- ln2_b: float32 [2, 512], P(None, ('tp', 'fsdp'))
- w_ch1: float32 [2, 512, 2048], P(None, 'fsdp', 'tp')
- b_ch1: float32 [2, 2048], P(None, ('tp', 'fsdp'))
- w_ch2: float32 [2, 2048, 512], P(None, ('tp', 'fsdp'))
- b_ch2: float32 [2, 512], P(None, ('tp', 'fsdp'))
- lnf_g: float32 [512], P(('tp', 'fsdp'))
- lnf_b: float32 [512], P(('tp', 'fsdp'))
- w_head: float32 [512, 1000], P('fsdp', 'tp')
- b_head: float32 [1000], P('tp')
Outputs:
- output 1: float32 [], replicated
- output 2: float32 [3072, 512], P('fsdp', 'tp')
- output 3: float32 [512], P(('tp', 'fsdp'))
- output 4: float32 [2, 512], P(None, ('tp', 'fsdp'))
- output 5: float32 [2, 512], P(None, ('tp', 'fsdp'))
- output 6: float32 [2, 49, 256], P(None, None, 'fsdp')
- output 7: float32 [2, 256], P(None, 'fsdp')
- output 8: float32 [2, 256, 49], P(None, 'fsdp')
- output 9: float32 [2, 512], P(None, ('tp', 'fsdp'))
- output 10: float32 [2, 512], P(None, ('tp', 'fsdp'))
- output 11: float32 [2, 512, 2048], P(None, 'fsdp', 'tp')
- output 12: float32 [2, 2048], P(None, ('tp', 'fsdp'))
- output 13: float32 [2, 2048, 512], P(None, ('tp', 'fsdp'))
- output 14: float32 [2, 512], P(None, ('tp', 'fsdp'))
- output 15: float32 [512], P(('tp', 'fsdp'))
- output 16: float32 [512], P(('tp', 'fsdp'))
- output 17: float32 [512, 1000], P('fsdp', 'tp')
- output 18: float32 [1000], P('tp')
All inputs are finite; a program needn't handle non-finite values.
Results may differ from the reference program's by a relative error of at most 0.0151881.
Values are sent between devices in bfloat16 or wider.
A program may use at most 1 GiB of HBM per device.

```python
import jax
import jax.numpy as jnp
from jax import lax

PATCH_SIDE = 32
TOKENS = 49
CHANNELS = 512
TOKEN_HIDDEN = 256
CHANNEL_HIDDEN = 2048
CLASSES = 1000
LAYERS = 2
IMAGES = 256
BLOCKS = 8

PATCH_DIM = 3 * PATCH_SIDE * PATCH_SIDE
PER_BLOCK = IMAGES // BLOCKS
EPS = 1e-6
LAYER_NAMES = ('ln1_g', 'ln1_b', 'w_tok1', 'b_tok1', 'w_tok2', 'ln2_g', 'ln2_b', 'w_ch1', 'b_ch1', 'w_ch2', 'b_ch2')


def setup_inputs(seed: int = 0) -> dict:
    key_list = jax.random.split(jax.random.key(seed), 20)

    def normal(index, shape, scale):
        return scale * jax.random.normal(key_list[index], shape, jnp.float32)

    chan_shape = (LAYERS, CHANNELS)
    return {
        'patches': normal(0, (IMAGES, TOKENS, PATCH_DIM), 1.0).astype(jnp.bfloat16),
        'labels': jax.random.randint(key_list[1], (IMAGES,), 0, CLASSES, jnp.int32),
        'w_stem': normal(2, (PATCH_DIM, CHANNELS), PATCH_DIM ** -0.5),
        'b_stem': normal(3, (CHANNELS,), 0.5),
        'ln1_g': 1.0 + normal(4, chan_shape, 0.3),
        'ln1_b': normal(5, chan_shape, 0.3),
        'w_tok1': normal(6, (LAYERS, TOKENS, TOKEN_HIDDEN), TOKENS ** -0.5),
        'b_tok1': normal(7, (LAYERS, TOKEN_HIDDEN), 0.3),
        'w_tok2': normal(8, (LAYERS, TOKEN_HIDDEN, TOKENS), TOKEN_HIDDEN ** -0.5),
        'ln2_g': 1.0 + normal(9, chan_shape, 0.3),
        'ln2_b': normal(10, chan_shape, 0.3),
        'w_ch1': normal(11, (LAYERS, CHANNELS, CHANNEL_HIDDEN), CHANNELS ** -0.5),
        'b_ch1': normal(12, (LAYERS, CHANNEL_HIDDEN), 0.3),
        'w_ch2': normal(13, (LAYERS, CHANNEL_HIDDEN, CHANNELS), CHANNEL_HIDDEN ** -0.5),
        'b_ch2': normal(14, chan_shape, 0.3),
        'lnf_g': 1.0 + normal(15, (CHANNELS,), 0.3),
        'lnf_b': normal(16, (CHANNELS,), 0.3),
        'w_head': normal(17, (CHANNELS, CLASSES), CHANNELS ** -0.5),
        'b_head': normal(18, (CLASSES,), 0.5),
    }


def as_matmul(values):
    return values.astype(jnp.bfloat16).astype(jnp.float32)


def layer_norm(values, gain, shift):
    mean_val = jnp.mean(values, axis=-1, keepdims=True)
    centered = values - mean_val
    var_val = jnp.mean(centered * centered, axis=-1, keepdims=True)
    return centered * lax.rsqrt(var_val + EPS) * gain + shift


def mixer_layer(resid, layer):
    normed = as_matmul(layer_norm(resid, layer['ln1_g'], layer['ln1_b']))
    hidden = jnp.einsum('bsc,sj->bcj', normed, as_matmul(layer['w_tok1'])) + layer['b_tok1']
    mixed = jnp.einsum('bcj,js->bsc', as_matmul(jax.nn.gelu(hidden)), as_matmul(layer['w_tok2']))
    resid = resid + mixed
    normed = as_matmul(layer_norm(resid, layer['ln2_g'], layer['ln2_b']))
    hidden = jnp.einsum('bsc,cd->bsd', normed, as_matmul(layer['w_ch1'])) + layer['b_ch1']
    out_val = jnp.einsum('bsd,dc->bsc', as_matmul(jax.nn.gelu(hidden)), as_matmul(layer['w_ch2']))
    return resid + out_val + layer['b_ch2'], None


def block_loss(weights, patch_blk, label_blk):
    resid = jnp.einsum('bsp,pc->bsc', patch_blk.astype(jnp.float32), as_matmul(weights['w_stem'])) + weights['b_stem']
    layer_weights = {name: weights[name] for name in LAYER_NAMES}
    resid = lax.scan(mixer_layer, resid, layer_weights)[0]
    pooled = jnp.mean(resid, axis=1)
    normed = as_matmul(layer_norm(pooled, weights['lnf_g'], weights['lnf_b']))
    logits = jnp.einsum('bc,ck->bk', normed, as_matmul(weights['w_head'])) + weights['b_head']
    log_norm = jax.nn.logsumexp(logits, axis=-1)
    class_ids = jnp.arange(CLASSES, dtype=jnp.int32)
    picked = jnp.sum(jnp.where(class_ids[None, :] == label_blk[:, None], logits, 0.0), axis=-1)
    return jnp.sum(log_norm - picked)


def reference(patches, labels, w_stem, b_stem, ln1_g, ln1_b, w_tok1, b_tok1, w_tok2,
              ln2_g, ln2_b, w_ch1, b_ch1, w_ch2, b_ch2, lnf_g, lnf_b, w_head, b_head):
    weights = dict(w_stem=w_stem, b_stem=b_stem, ln1_g=ln1_g, ln1_b=ln1_b, w_tok1=w_tok1,
                   b_tok1=b_tok1, w_tok2=w_tok2, ln2_g=ln2_g, ln2_b=ln2_b, w_ch1=w_ch1,
                   b_ch1=b_ch1, w_ch2=w_ch2, b_ch2=b_ch2, lnf_g=lnf_g, lnf_b=lnf_b,
                   w_head=w_head, b_head=b_head)
    patch_blocks = patches.reshape(BLOCKS, PER_BLOCK, TOKENS, PATCH_DIM)
    label_blocks = labels.reshape(BLOCKS, PER_BLOCK)
    loss_grad = jax.value_and_grad(block_loss)

    def accumulate(carry, block):
        loss_sum, grad_sum = carry
        value, grads = loss_grad(weights, block[0], block[1])
        return (loss_sum + value, jax.tree.map(jnp.add, grad_sum, grads)), None

    start_carry = (jnp.zeros((), jnp.float32), jax.tree.map(jnp.zeros_like, weights))
    loss_sum, grad_sum = lax.scan(accumulate, start_carry, (patch_blocks, label_blocks))[0]
    scale = 1.0 / IMAGES
    return (loss_sum * scale, grad_sum['w_stem'] * scale, grad_sum['b_stem'] * scale,
            grad_sum['ln1_g'] * scale, grad_sum['ln1_b'] * scale, grad_sum['w_tok1'] * scale,
            grad_sum['b_tok1'] * scale, grad_sum['w_tok2'] * scale, grad_sum['ln2_g'] * scale,
            grad_sum['ln2_b'] * scale, grad_sum['w_ch1'] * scale, grad_sum['b_ch1'] * scale,
            grad_sum['w_ch2'] * scale, grad_sum['b_ch2'] * scale, grad_sum['lnf_g'] * scale,
            grad_sum['lnf_b'] * scale, grad_sum['w_head'] * scale, grad_sum['b_head'] * scale)
```

```python
import functools

import jax
import jax.numpy as jnp
from jax import lax
from jax.experimental import pallas as pl
from jax.experimental.pallas import tpu as pltpu
from jax.sharding import PartitionSpec as P

EPS = 1e-6
CHANNEL_AXES = ('tp', 'fsdp')
LAYER_NAMES = ('ln1_g', 'ln1_b', 'w_tok1', 'b_tok1', 'w_tok2', 'ln2_g', 'ln2_b', 'w_ch1', 'b_ch1', 'w_ch2', 'b_ch2')
MESH = pl.DeviceIdType.MESH
BF16 = jnp.bfloat16
F32 = jnp.float32
ORDERS = ((0, 1, 2), (1, 2, 0), (2, 0, 1))


def product(form, left, right):
    return jnp.einsum(form, left, right, preferred_element_type=jnp.float32)


def my_position():
    tp, fsdp = lax.axis_index('tp'), lax.axis_index('fsdp')
    return (lax.rem(fsdp // 2, 2), fsdp // 4, tp), lax.rem(fsdp, 2)


def shifted(coords, bits):
    return tuple(1 - c if b else c for c, b in zip(coords, bits))


def owner_of(coords, core):
    x, y, z = coords
    return z, y * 4 + x * 2 + core


def device_of(coords, core):
    tp, fsdp = owner_of(coords, core)
    return {'tp': tp, 'fsdp': fsdp}


def unit(dim):
    return tuple(1 if d == dim else 0 for d in range(3))


def plus(a, b):
    return tuple((i + j) % 2 for i, j in zip(a, b))


def entry_barrier(coords, core):
    barrier = pltpu.get_barrier_semaphore()
    for dim in range(3):
        pl.semaphore_signal(barrier, inc=1, device_id=device_of(shifted(coords, unit(dim)), core), device_id_type=MESH)
    pl.semaphore_signal(barrier, inc=1, device_id=device_of(coords, 1 - core), device_id_type=MESH)
    pl.semaphore_wait(barrier, 4)


def stem_block(ref, tp, fsdp, lo, num):
    return ref.at[pl.ds(pl.multiple_of(fsdp * 384 + lo, 16), num), pl.ds(pl.multiple_of(tp * 256, 128), 256)]


def ch1_block(ref, tp, fsdp, lo, num):
    return ref.at[:, pl.ds(pl.multiple_of(fsdp * 64 + lo, 8), num), pl.ds(pl.multiple_of(tp * 1024, 128), 1024)]


def ch2_block(ref, tp, fsdp, lo, num):
    return ref.at[:, pl.ds(pl.multiple_of((tp * 8 + fsdp) * 128 + lo, 8), num), :]


def head_block(ref, tp, fsdp, lo, num):
    return ref.at[pl.ds(pl.multiple_of(fsdp * 64 + lo, 8), num), pl.ds(pl.multiple_of(tp * 512, 128), 512)]


def small_block(ref, tp, fsdp, lo, num):
    return ref.at[tp * 8 + fsdp, pl.ds(lo, num), :]


BLOCKS = (stem_block, small_block, ch1_block, ch2_block, head_block)
GATHER_SPLITS = (((0, 128), (128, 128), (256, 128)), ((0, 24), (24, 24), (48, 16)),
                 ((0, 16), (16, 16), (32, 32)), ((0, 48), (48, 48), (96, 32)), ((0, 32), (32, 16), (48, 16)))
LAYERED = (False, False, True, True, False)


def rows_of(ref, layered, lo, num):
    return ref.at[:, pl.ds(lo, num), :] if layered else ref.at[pl.ds(lo, num), :]


def gather_kernel(*refs):
    own, full = refs[:5], refs[5:10]
    send_sem, recv_sem, local_sem = refs[10:]
    coords, core = my_position()
    entry_barrier(coords, core)
    pending = []

    def move(item, part, bits, src_is_own, target_coords, target_core, sem_index):
        lo, num = GATHER_SPLITS[item][part]
        tp, fsdp = owner_of(shifted(coords, bits), core)
        there = BLOCKS[item](full[item], tp, fsdp, lo, num)
        here = rows_of(own[item], LAYERED[item], lo, num) if src_is_own else there
        copy = pltpu.make_async_remote_copy(
            src_ref=here, dst_ref=there, send_sem=send_sem, recv_sem=recv_sem.at[item, part, sem_index],
            device_id=device_of(target_coords, target_core), device_id_type=MESH)
        copy.start()
        pending.append(copy)

    def arrival(item, part, bits, from_core, sem_index):
        lo, num = GATHER_SPLITS[item][part]
        tp, fsdp = owner_of(shifted(coords, bits), from_core)
        there = BLOCKS[item](full[item], tp, fsdp, lo, num)
        pltpu.make_async_remote_copy(
            src_ref=there, dst_ref=there, send_sem=send_sem, recv_sem=recv_sem.at[item, part, sem_index],
            device_id=device_of(coords, core), device_id_type=MESH).wait_recv()

    def pass_on(item, part, bits, level):
        order = ORDERS[part]
        rank = sum(2 ** i for i in range(3) if bits[order[i]])
        for step in range(level, 3):
            target = shifted(coords, unit(order[step]))
            move(item, part, bits, level == 0, target, core, (0, 1, 3)[step] + rank)
        move(item, part, bits, level == 0, coords, 1 - core, 7 + rank)

    for item in range(5):
        for part in range(3):
            pass_on(item, part, (0, 0, 0), 0)
    locals_ = []
    for item in range(5):
        tp, fsdp = owner_of(coords, core)
        nrows = own[item].shape[-2]
        copy = pltpu.make_async_copy(own[item], BLOCKS[item](full[item], tp, fsdp, 0, nrows), local_sem.at[item])
        copy.start()
        locals_.append(copy)
    for level in range(3):
        for item in range(5):
            for part in range(3):
                order = ORDERS[part]
                for sub in range(2 ** level):
                    bits = [0, 0, 0]
                    for i in range(level):
                        if (sub >> i) % 2:
                            bits[order[i]] = 1
                    arrived = plus(tuple(bits), unit(order[level]))
                    arrival(item, part, arrived, core, (0, 1, 3)[level] + sub)
                    pass_on(item, part, arrived, level + 1)
    for item in range(5):
        for part in range(3):
            order = ORDERS[part]
            for rank in range(8):
                bits = [0, 0, 0]
                for i in range(3):
                    if (rank >> i) % 2:
                        bits[order[i]] = 1
                arrival(item, part, tuple(bits), 1 - core, 7 + rank)
    for copy in locals_:
        copy.wait()
    for copy in pending:
        copy.wait_send()


def gather_all(own):
    any_spec = pl.BlockSpec(memory_space=pl.ANY)
    shapes = [jax.ShapeDtypeStruct((3072, 512), BF16), jax.ShapeDtypeStruct((16, 64, 128), F32),
              jax.ShapeDtypeStruct((2, 512, 2048), BF16), jax.ShapeDtypeStruct((2, 2048, 512), BF16),
              jax.ShapeDtypeStruct((512, 1024), BF16)]
    return pl.pallas_call(
        gather_kernel, out_shape=shapes, in_specs=[any_spec] * 5, out_specs=[any_spec] * 5,
        scratch_shapes=[pltpu.SemaphoreType.DMA, pltpu.SemaphoreType.DMA((5, 3, 15)), pltpu.SemaphoreType.DMA((5,))],
        compiler_params=pltpu.CompilerParams(collective_id=0, has_side_effects=True),
        cost_estimate=pl.CostEstimate(flops=10 ** 9, bytes_accessed=25 * 10 ** 6, transcendentals=0),
        name='gather_weights')(*own)


SUM_SPLITS = (((0, 128), (128, 128), (256, 128)), ((0, 24), (24, 24), (48, 16)),
              ((0, 24), (24, 24), (48, 16)), ((0, 40), (40, 40), (80, 48)), ((0, 24), (24, 24), (48, 16)))
SUM_SHAPES = ((384, 256), (64, 128), (2, 64, 1024), (2, 128, 512), (64, 512))
SUM_ORDER = (4, 3, 2, 0, 1)


BOTH = range(2)


def all_bits():
    return [(x, y, z) for z in BOTH for y in BOTH for x in BOTH]


def sum_kernel(*refs):
    full, out = refs[:5], refs[5:10]
    mine, peer = refs[10:15], refs[15:20]
    inbox = refs[20:65]
    send_sem, peer_sem, load_sem, recv_sem = refs[65:]
    coords, core = my_position()
    entry_barrier(coords, core)
    pending = []
    loads = {}

    def box(item, part, phase):
        return inbox[item * 9 + part * 3 + phase]

    for item in SUM_ORDER:
        for index, bits in enumerate(all_bits()):
            x, y, z = bits
            tp, fsdp = owner_of(shifted(coords, bits), 1 - core)
            nrows = SUM_SHAPES[item][-2]
            copy = pltpu.make_async_remote_copy(
                src_ref=BLOCKS[item](full[item], tp, fsdp, 0, nrows), dst_ref=peer[item].at[z, y, x],
                send_sem=send_sem, recv_sem=peer_sem.at[item, index],
                device_id=device_of(coords, 1 - core), device_id_type=MESH)
            copy.start()
            pending.append(copy)
            tp, fsdp = owner_of(shifted(coords, bits), core)
            load = pltpu.make_async_copy(BLOCKS[item](full[item], tp, fsdp, 0, nrows), mine[item].at[z, y, x],
                                         load_sem.at[item, index])
            load.start()
            loads[item, index] = (copy, load)

    def view(ref, item, part, select):
        lo, num = SUM_SPLITS[item][part]
        z, y, x = select[2], select[1], select[0]
        if LAYERED[item]:
            return ref.at[z, y, x, :, pl.ds(lo, num), :]
        return ref.at[z, y, x, pl.ds(lo, num), :]

    def send_phase(item, part, phase):
        order = ORDERS[part]
        select = [slice(None)] * 3
        for i in range(phase):
            select[order[i]] = 0
        select[order[phase]] = 1
        copy = pltpu.make_async_remote_copy(
            src_ref=view(mine[item], item, part, select), dst_ref=box(item, part, phase),
            send_sem=send_sem, recv_sem=recv_sem.at[item, part, phase],
            device_id=device_of(shifted(coords, unit(order[phase])), core), device_id_type=MESH)
        copy.start()
        pending.append(copy)
        return copy

    copies = {}
    for item in SUM_ORDER:
        for index in range(8):
            copy, load = loads[item, index]
            load.wait()
            copy.wait_recv()

        @pl.loop(0, 8)
        def _(i):
            z, y, x = i // 4, lax.rem(i // 2, 2), lax.rem(i, 2)
            mine[item][z, y, x] = mine[item][z, y, x] + peer[item][z, y, x]
        for part in range(3):
            copies[item, part, 0] = send_phase(item, part, 0)
    for phase in range(3):
        for item in SUM_ORDER:
            for part in range(3):
                copies[item, part, phase].wait_recv()
                order = ORDERS[part]
                rest = [d for d in range(3) if d not in order[:phase + 1]]
                select = [0, 0, 0]
                buf = box(item, part, phase)
                for sub in range(2 ** len(rest)):
                    where = list(select)
                    index = []
                    for j, d in enumerate(sorted(rest, reverse=True)):
                        bit = (sub >> j) % 2
                        where[d] = bit
                        index.append(bit)
                    dst = view(mine[item], item, part, where)
                    src = buf.at[tuple(index)] if index else buf
                    dst[...] = dst[...] + src[...]
                if phase < 2:
                    copies[item, part, phase + 1] = send_phase(item, part, phase + 1)
    for item in range(5):
        out[item][...] = mine[item][0, 0, 0]
    for copy in pending:
        copy.wait_send()


def sum_all(full):
    any_spec = pl.BlockSpec(memory_space=pl.ANY)
    vmem = pl.BlockSpec(memory_space=pltpu.VMEM)
    boxes = []
    for item in range(5):
        for part in range(3):
            num = SUM_SPLITS[item][part][1]
            shape = SUM_SHAPES[item][:-2] + (num, SUM_SHAPES[item][-1])
            for phase in range(3):
                boxes.append(pltpu.VMEM((2,) * (2 - phase) + shape, F32))
    slots = [pltpu.VMEM((2, 2, 2) + s, F32) for s in SUM_SHAPES]
    return pl.pallas_call(
        sum_kernel, out_shape=[jax.ShapeDtypeStruct(s, F32) for s in SUM_SHAPES],
        in_specs=[any_spec] * 5, out_specs=[vmem] * 5,
        scratch_shapes=slots + slots + boxes + [
            pltpu.SemaphoreType.DMA, pltpu.SemaphoreType.DMA((5, 8)), pltpu.SemaphoreType.DMA((5, 8)),
            pltpu.SemaphoreType.DMA((5, 3, 3))],
        compiler_params=pltpu.CompilerParams(collective_id=1, has_side_effects=True, vmem_limit_bytes=63 * 2 ** 20),
        cost_estimate=pl.CostEstimate(flops=10 ** 9, bytes_accessed=50 * 10 ** 6, transcendentals=0),
        name='sum_gradients')(*full)


VECTORS = (('b_stem', 1), ('lnf_g', 1), ('lnf_b', 1), ('ln1_g', 2), ('ln1_b', 2), ('ln2_g', 2), ('ln2_b', 2), ('b_ch2', 2))


def pack_own(weights):
    pieces = [weights[name].reshape(-1) for name, _ in VECTORS]
    pieces += [weights[name].reshape(-1) for name in ('b_ch1', 'b_tok1', 'w_tok1', 'w_tok2', 'b_head')]
    flat = jnp.concatenate(pieces)
    return jnp.pad(flat, (0, 8192 - flat.shape[0])).reshape(64, 128)


def unpack_full(packed):
    rows = packed.reshape(16, 8192)
    found = {}
    at = 0
    for name, num in VECTORS:
        found[name] = rows[:, at:at + num * 32].reshape(16, num, 32).swapaxes(0, 1).reshape(num, 512)
        at += num * 32
    found['b_ch1'] = rows[:, at:at + 256].reshape(16, 2, 128).swapaxes(0, 1).reshape(2, 2048)
    at += 256
    half = rows[:8]
    found['b_tok1'] = half[:, at:at + 64].reshape(8, 2, 32).swapaxes(0, 1).reshape(2, 256)
    at += 64
    found['w_tok1'] = half[:, at:at + 3136].reshape(8, 2, 49, 32).transpose(1, 2, 0, 3).reshape(2, 49, 256)
    at += 3136
    found['w_tok2'] = half[:, at:at + 3136].reshape(8, 2, 32, 49).swapaxes(0, 1).reshape(2, 256, 49)
    at += 3136
    found['b_head'] = jnp.pad(rows[::8, at:at + 500], ((0, 0), (0, 12))).reshape(1024)
    return found


def pack_grads(grads, loss):
    pieces = [grads[name].reshape(num, 16, 32).swapaxes(0, 1).reshape(16, num * 32) for name, num in VECTORS]
    pieces.append(grads['b_ch1'].reshape(2, 16, 128).swapaxes(0, 1).reshape(16, 256))

    def twice(values):
        return jnp.concatenate([values, values], axis=0)
    pieces.append(twice(grads['b_tok1'].reshape(2, 8, 32).swapaxes(0, 1).reshape(8, 64)))
    pieces.append(twice(grads['w_tok1'].reshape(2, 49, 8, 32).transpose(2, 0, 1, 3).reshape(8, 3136)))
    pieces.append(twice(grads['w_tok2'].reshape(2, 8, 32, 49).swapaxes(0, 1).reshape(8, 3136)))
    pieces.append(jnp.repeat(grads['b_head'].reshape(2, 512)[:, :500], 8, axis=0))
    pieces.append(jnp.broadcast_to(loss.reshape(1, 1), (16, 1)))
    flat = jnp.concatenate(pieces, axis=1)
    return jnp.pad(flat, ((0, 0), (0, 8192 - flat.shape[1]))).reshape(16, 64, 128)


def unpack_own(packed):
    flat = packed.reshape(-1)
    found = {}
    at = 0
    for name, num in VECTORS:
        found[name] = flat[at:at + num * 32].reshape((num, 32) if num == 2 else (32,))
        at += num * 32
    for name, shape in (('b_ch1', (2, 128)), ('b_tok1', (2, 32)), ('w_tok1', (2, 49, 32)), ('w_tok2', (2, 32, 49)),
                        ('b_head', (500,)), ('loss', ())):
        size = 1
        for s in shape:
            size *= s
        found[name] = flat[at:at + size].reshape(shape)
        at += size
    return found


def norm_forward(values, gain, shift):
    mean_val = jnp.mean(values, axis=-1, keepdims=True)
    centered = values - mean_val
    inv_std = lax.rsqrt(jnp.mean(centered * centered, axis=-1, keepdims=True) + EPS)
    standard = centered * inv_std
    return standard * gain + shift, standard, inv_std


def norm_backward(grad_out, gain, standard, inv_std):
    grad_std = grad_out * gain
    first = jnp.mean(grad_std, axis=-1, keepdims=True)
    second = jnp.mean(grad_std * standard, axis=-1, keepdims=True)
    return inv_std * (grad_std - first - standard * second)


def gelu_grad(pre_act, grad_out):
    return jax.vjp(jax.nn.gelu, pre_act)[1](grad_out)[0]


def lead_sum(values):
    return jnp.sum(values.reshape(-1, values.shape[-1]), axis=0)


def weight_specs():
    vec_spec = P(CHANNEL_AXES)
    layer_vec = P(None, CHANNEL_AXES)
    return (P('fsdp', 'tp'), vec_spec, layer_vec, layer_vec, P(None, None, 'fsdp'), P(None, 'fsdp'),
            P(None, 'fsdp', None), layer_vec, layer_vec, P(None, 'fsdp', 'tp'), layer_vec,
            P(None, CHANNEL_AXES, None), layer_vec, vec_spec, vec_spec, P('fsdp', 'tp'), P('tp'))


def solution(mesh):
    total_images = 256

    def step(patches, labels, w_stem, b_stem, ln1_g, ln1_b, w_tok1, b_tok1, w_tok2,
             ln2_g, ln2_b, w_ch1, b_ch1, w_ch2, b_ch2, lnf_g, lnf_b, w_head, b_head):
        half = patches.shape[0] // 2
        tp = lax.axis_index('tp')
        patches = lax.dynamic_slice_in_dim(patches, tp * half, half, 0)
        labels = lax.dynamic_slice_in_dim(labels, tp * half, half, 0)
        small_own = pack_own(dict(b_stem=b_stem, lnf_g=lnf_g, lnf_b=lnf_b, ln1_g=ln1_g, ln1_b=ln1_b, ln2_g=ln2_g,
                                  ln2_b=ln2_b, b_ch2=b_ch2, b_ch1=b_ch1, b_tok1=b_tok1, w_tok1=w_tok1, w_tok2=w_tok2,
                                  b_head=b_head))
        head_own = jnp.pad(w_head.astype(BF16), ((0, 0), (0, 12)))
        stem_w, small, ch1_w, ch2_w, head_w = gather_all(
            [w_stem.astype(BF16), small_own, w_ch1.astype(BF16), w_ch2.astype(BF16), head_own])
        small = unpack_full(small)
        tok1_w, tok2_w = small['w_tok1'].astype(BF16), small['w_tok2'].astype(BF16)

        tokens = patches.shape[1]
        resid = product('bsp,pc->bsc', patches, stem_w) + small['b_stem'][0]
        saved = []
        for layer in range(2):
            normed, norm1_std, norm1_inv = norm_forward(resid, small['ln1_g'][layer], small['ln1_b'][layer])
            normed = normed.astype(BF16)
            tok_pre = product('bsc,sj->bjc', normed, tok1_w[layer]) + small['b_tok1'][layer][:, None]
            tok_act = jax.nn.gelu(tok_pre).astype(BF16)
            resid = resid + product('bjc,js->bsc', tok_act, tok2_w[layer])
            normed2, norm2_std, norm2_inv = norm_forward(resid, small['ln2_g'][layer], small['ln2_b'][layer])
            full_in = normed2.astype(BF16)
            ch_pre = product('bsc,cd->bsd', full_in, ch1_w[layer]) + small['b_ch1'][layer]
            ch_act = jax.nn.gelu(ch_pre).astype(BF16)
            resid = resid + product('bsd,dc->bsc', ch_act, ch2_w[layer]) + small['b_ch2'][layer]
            saved.append(dict(normed=normed, norm1_std=norm1_std, norm1_inv=norm1_inv, tok_pre=tok_pre,
                              tok_act=tok_act, norm2_std=norm2_std, norm2_inv=norm2_inv,
                              full_in=full_in, ch_pre=ch_pre, ch_act=ch_act))

        pooled = jnp.mean(resid, axis=1)
        head_in, head_std, head_inv = norm_forward(pooled, small['lnf_g'][0], small['lnf_b'][0])
        head_full = head_in.astype(BF16)
        logits = product('bc,ck->bk', head_full, head_w) + small['b_head']
        column = lax.broadcasted_iota(jnp.int32, logits.shape, 1)
        real = lax.rem(column, 512) < 500
        class_ids = (column // 512) * 500 + lax.rem(column, 512)
        is_label = jnp.logical_and(class_ids == labels[:, None], real)
        row_max = jnp.max(jnp.where(real, logits, -jnp.inf), axis=1, keepdims=True)
        exps = jnp.where(real, jnp.exp(jnp.where(real, logits, row_max) - row_max), 0.0)
        sums = jnp.sum(exps, axis=1, keepdims=True)
        picked = jnp.sum(jnp.where(is_label, logits, 0.0), axis=1)
        loss = jnp.sum(row_max[:, 0] + jnp.log(sums[:, 0]) - picked) / total_images

        grads = {}
        d_logits = (exps / sums - is_label.astype(F32)) / total_images
        d_logits_bf = d_logits.astype(BF16)
        g_head = product('bc,bk->ck', head_full, d_logits_bf)
        grads['b_head'] = jnp.sum(d_logits, axis=0)
        d_head_in = product('bk,ck->bc', d_logits_bf, head_w)
        grads['lnf_g'] = jnp.sum(d_head_in * head_std, axis=0)
        grads['lnf_b'] = jnp.sum(d_head_in, axis=0)
        d_pooled = norm_backward(d_head_in, small['lnf_g'][0], head_std, head_inv)
        d_resid = jnp.broadcast_to((d_pooled / tokens)[:, None, :], resid.shape)

        lists = {name: [] for name in LAYER_NAMES}
        for layer in (1, 0):
            keep = saved[layer]
            lists['b_ch2'].append(lead_sum(d_resid))
            d_out = d_resid.astype(BF16)
            lists['w_ch2'].append(product('bsd,bsc->dc', keep['ch_act'], d_out))
            d_ch_pre = gelu_grad(keep['ch_pre'], product('bsc,dc->bsd', d_out, ch2_w[layer]))
            lists['b_ch1'].append(lead_sum(d_ch_pre))
            d_ch_pre_bf = d_ch_pre.astype(BF16)
            lists['w_ch1'].append(product('bsc,bsd->cd', keep['full_in'], d_ch_pre_bf))
            d_norm2 = product('bsd,cd->bsc', d_ch_pre_bf, ch1_w[layer])
            lists['ln2_g'].append(lead_sum(d_norm2 * keep['norm2_std']))
            lists['ln2_b'].append(lead_sum(d_norm2))
            d_mid = d_resid + norm_backward(d_norm2, small['ln2_g'][layer], keep['norm2_std'], keep['norm2_inv'])
            d_mid_bf = d_mid.astype(BF16)
            lists['w_tok2'].append(product('bjc,bsc->js', keep['tok_act'], d_mid_bf))
            d_tok_pre = gelu_grad(keep['tok_pre'], product('bsc,js->bjc', d_mid_bf, tok2_w[layer]))
            lists['b_tok1'].append(jnp.sum(d_tok_pre, axis=(0, 2)))
            d_tok_pre_bf = d_tok_pre.astype(BF16)
            lists['w_tok1'].append(product('bsc,bjc->sj', keep['normed'], d_tok_pre_bf))
            d_norm1 = product('bjc,sj->bsc', d_tok_pre_bf, tok1_w[layer])
            lists['ln1_g'].append(lead_sum(d_norm1 * keep['norm1_std']))
            lists['ln1_b'].append(lead_sum(d_norm1))
            d_resid = d_mid + norm_backward(d_norm1, small['ln1_g'][layer], keep['norm1_std'], keep['norm1_inv'])

        grads['b_stem'] = lead_sum(d_resid)
        g_stem = product('bsp,bsc->pc', patches, d_resid.astype(BF16))
        for name in LAYER_NAMES:
            grads[name] = jnp.stack(lists[name][::-1])
        o_stem, o_small, o_ch1, o_ch2, o_head = sum_all(
            [g_stem, pack_grads(grads, loss), grads['w_ch1'], grads['w_ch2'], g_head])
        found = unpack_own(o_small)
        found['w_ch1'], found['w_ch2'] = o_ch1, o_ch2
        return tuple([found['loss'], o_stem, found['b_stem']] + [found[name] for name in LAYER_NAMES]
                     + [found['lnf_g'], found['lnf_b'], o_head[:, :500], found['b_head']])

    specs = weight_specs()
    return jax.shard_map(step, mesh=mesh, in_specs=(P('fsdp', None, None), P('fsdp')) + specs,
                         out_specs=(P(),) + specs, check_vma=False)
```

```python
import functools

import jax
import jax.numpy as jnp
from jax import lax
from jax.experimental import pallas as pl
from jax.experimental.pallas import tpu as pltpu
from jax.sharding import PartitionSpec as P

EPS = 1e-6
CHANNEL_AXES = ('tp', 'fsdp')
LAYER_NAMES = ('ln1_g', 'ln1_b', 'w_tok1', 'b_tok1', 'w_tok2', 'ln2_g', 'ln2_b', 'w_ch1', 'b_ch1', 'w_ch2', 'b_ch2')
N0, N1, N2, N3, N4, N5, N6, N7, N8 = range(9)
MESH = pl.DeviceIdType.MESH
BF16 = jnp.bfloat16
F32 = jnp.float32
ORDERS = ((N0, N1, N2), (N1, N2, N0), (N2, N0, N1))


def my_position():
    tp, fsdp = lax.axis_index('tp'), lax.axis_index('fsdp')
    return (lax.rem(fsdp // N2, N2), fsdp // N4, tp), lax.rem(fsdp, N2)


def aligned(value, size):
    return value if isinstance(value, int) else pl.multiple_of(value, size)


def odd(value):
    return value % N2 if isinstance(value, int) else lax.rem(value, N2)


def shifted(coords, bits):
    return tuple(N1 - c if b else c for c, b in zip(coords, bits))


def owner_of(coords, core):
    x, y, z = coords
    return z, y * N4 + x * N2 + core


def device_of(coords, core):
    tp, fsdp = owner_of(coords, core)
    return {'tp': tp, 'fsdp': fsdp}


def unit(dim):
    return tuple(N1 if d == dim else N0 for d in range(N3))


def plus(a, b):
    return tuple((i + j) % N2 for i, j in zip(a, b))


def entry_barrier(coords, core):
    barrier = pltpu.get_barrier_semaphore()
    for dim in range(N3):
        pl.semaphore_signal(barrier, inc=N1, device_id=device_of(shifted(coords, unit(dim)), core), device_id_type=MESH)
    pl.semaphore_signal(barrier, inc=N1, device_id=device_of(coords, N1 - core), device_id_type=MESH)
    pl.semaphore_wait(barrier, N4)


ROW_VEC = dict(b_stem=N0, ln1_g=N1, ln1_b=N3, ln2_g=N5, ln2_b=N7, b_ch2=9, b_ch1=11, lnf_g=19, lnf_b=20, b_head=21, loss=23)
VEC_ROWS = 24
TOK = 56
IMAGES = 16
ROWS = TOK * IMAGES
BAND = 128
BANDS = ROWS // BAND
WIDE = 512
DEEP = 2048
HALF = ROWS // N2
GELU_A = 0.7978845608028654
GELU_B = 0.044715


def by_rows(left, right):
    return lax.dot_general(left, right, (((N1,), (N1,)), ((), ())), preferred_element_type=F32)


def times(left, right):
    return jnp.dot(left, right, preferred_element_type=F32)


def gelu_pair(pre):
    square = pre * pre
    tanh = jnp.tanh(GELU_A * (pre + GELU_B * (square * pre)))
    cdf = 0.5 + 0.5 * tanh
    slope = cdf + (0.5 * pre) * (1.0 - tanh * tanh) * (GELU_A + (3.0 * GELU_A * GELU_B) * square)
    return pre * cdf, slope


def standardize(values):
    centered = values - jnp.mean(values, axis=N1, keepdims=True)
    inv_std = lax.rsqrt(jnp.mean(centered * centered, axis=N1, keepdims=True) + EPS)
    return centered * inv_std, inv_std


def norm_back(grad_out, gain, standard, inv_std):
    grad_std = grad_out * gain
    first = jnp.mean(grad_std, axis=N1, keepdims=True)
    second = jnp.mean(grad_std * standard, axis=N1, keepdims=True)
    return inv_std * (grad_std - first - standard * second)


def row_sum(values):
    return jnp.sum(values, axis=N0, keepdims=True)


DIMS = range(N3)


STEM_W, SMALL, HEAD_W, CHAN1, CHAN2 = N0, N1, N6, (N2, N4), (N3, N5)
GATHER_SPLITS = (((N0, 128), (128, 128), (256, 128)), ((N0, 72), (72, 64), (136, 64)),
                 ((N0, 16), (16, 16), (32, 32)), ((N0, 48), (48, 48), (96, 32)),
                 ((N0, 16), (16, 16), (32, 32)), ((N0, 48), (48, 48), (96, 32)), ((N0, 32), (32, 16), (48, 16)))
GATHERED = len(GATHER_SPLITS)
PACK_ROWS = 200
AT_B1, AT_BT, AT_BH, AT_T1, AT_T2 = 16, 18, 20, 24, 136
VECTORS = (('b_stem', N1), ('ln1_g', N2), ('ln1_b', N2), ('ln2_g', N2), ('ln2_b', N2), ('b_ch2', N2), ('lnf_g', N1), ('lnf_b', N1))
CLASSES_HALF = 500
TOKENS = 49
TOTAL = 256
PATCH = 3072


def forward_kernel(*refs):
    take = iter(refs)

    def grab(count):
        return [next(take) for _ in range(count)]
    patch_hbm, labels, f_stem, f1, f2, f_head = grab(N6)
    vec_in = grab(len(VECTORS))
    i_b1, i_bt, i_bh, i_t1, i_t2 = grab(N5)
    w1_out, w2_out, xa_out, xb_out, patch_out, t1t, t1, t2, bt, vec, gh, hs, d0 = grab(13)
    own_stem, own1, own2, own_head, pack = grab(N5)
    stem_w, small, w1, w2, head_w = grab(N5)
    pin, padded, pbuf, t2t = grab(N4)
    xs = grab(N5)
    v, pre, act, pooled = grab(N4)
    send_sem, recv_sem, load_sem, save_sem = grab(N4)
    coords, core = my_position()
    tp = coords[N2]
    half_images = pin.shape[N0]
    loads = []
    for b in range(half_images):
        copy = pltpu.make_async_copy(patch_hbm.at[tp * half_images + b], pin.at[b], load_sem.at[b])
        copy.start()
        loads.append(copy)

    own_stem[...] = f_stem[...].astype(BF16)
    own1[...] = f1[...].astype(BF16)
    own2[...] = f2[...].astype(BF16)
    own_head[...] = jnp.zeros(own_head.shape, BF16)
    own_head[:, :CLASSES_HALF] = f_head[...].astype(BF16)
    pack[...] = jnp.zeros(pack.shape, F32)
    row = N0
    for ref, (_, num) in zip(vec_in, VECTORS):
        pack[row:row + num, :32] = ref[...]
        row += num
    pack[AT_B1:AT_B1 + N2, :] = i_b1[...]
    pack[AT_BT:AT_BT + N2, :32] = i_bt[...]
    for k in range(N4):
        width = min(BAND, CLASSES_HALF - k * BAND)
        pack[AT_BH + k:AT_BH + k + N1, :width] = i_bh[:, k * BAND:k * BAND + width]
    for layer in range(N2):
        pack[AT_T1 + TOK * layer:AT_T1 + TOK * layer + TOKENS, :32] = i_t1[layer]
        pack[AT_T2 + 32 * layer:AT_T2 + 32 * layer + 32, :TOKENS] = i_t2[layer]
    entry_barrier(coords, core)

    own = [own_stem, pack, own1.at[N0], own2.at[N0], own1.at[N1], own2.at[N1], own_head]

    def block(item, tp, fsdp, lo, num):
        if item == STEM_W:
            return stem_w.at[pl.ds(aligned(fsdp * 384 + lo, 128), num), pl.ds(aligned(tp * 256, 128), 256)]
        if item == SMALL:
            return small.at[tp * N8 + fsdp, pl.ds(lo, num), :]
        if item in CHAN1:
            return w1.at[CHAN1.index(item), pl.ds(aligned(fsdp * 64 + lo, 16), num), pl.ds(aligned(tp * 1024, 128), 1024)]
        if item in CHAN2:
            return w2.at[CHAN2.index(item), pl.ds(aligned((tp * N8 + fsdp) * 128 + lo, 16), num), :]
        return head_w.at[pl.ds(aligned(fsdp * 64 + lo, 16), num), pl.ds(aligned(tp * WIDE, 128), WIDE)]

    def move(item, part, bits, is_own, target, slot):
        lo, num = GATHER_SPLITS[item][part]
        there = block(item, *owner_of(shifted(coords, bits), core), lo, num)
        here = own[item].at[pl.ds(lo, num), :] if is_own else there
        pltpu.make_async_remote_copy(src_ref=here, dst_ref=there, send_sem=send_sem,
                                     recv_sem=recv_sem.at[item, part, slot], device_id=target,
                                     device_id_type=MESH).start()

    def arrival(item, part, bits, from_core, slot):
        lo, num = GATHER_SPLITS[item][part]
        there = block(item, *owner_of(shifted(coords, bits), from_core), lo, num)
        pltpu.make_async_remote_copy(src_ref=there, dst_ref=there, send_sem=send_sem,
                                     recv_sem=recv_sem.at[item, part, slot], device_id=device_of(coords, core),
                                     device_id_type=MESH).wait_recv()

    def pass_on(item, part, bits, level):
        order = ORDERS[part]
        rank = sum(N2 ** i for i in DIMS if bits[order[i]])
        for step in range(level, N3):
            move(item, part, bits, level == N0, device_of(shifted(coords, unit(order[step])), core),
                 N2 ** step - N1 + rank)
        move(item, part, bits, level == N0, device_of(coords, N1 - core), N7 + rank)

    def bits_of(part, rank):
        bits = [N0, N0, N0]
        for i in DIMS:
            bits[ORDERS[part][i]] = (rank >> i) % N2
        return tuple(bits)

    def send_own(item):
        for part in DIMS:
            pass_on(item, part, (N0, N0, N0), N0)

    def forward(item, level):
        for part in DIMS:
            for rank in range(N2 ** level):
                bits = bits_of(part, rank + N2 ** level)
                arrival(item, part, bits, core, N2 ** level - N1 + rank)
                pass_on(item, part, bits, level + N1)

    def finish(item):
        for part in DIMS:
            for rank in range(N8):
                arrival(item, part, bits_of(part, rank), N1 - core, N7 + rank)

    def place_own(item):
        here = own[item]
        block(item, *owner_of(coords, core), N0, here.shape[N0])[...] = here[...]

    saves = []

    def save(src, dst):
        copy = pltpu.make_async_copy(src, dst, save_sem.at[len(saves)])
        copy.start()
        saves.append((src, dst))

    early = (STEM_W, SMALL)
    for item in early:
        send_own(item)
    send_own(CHAN1[N0])
    for item in range(GATHERED):
        place_own(item)
    padded[...] = jnp.zeros(padded.shape, F32)
    for item in early:
        forward(item, N0)
    send_own(CHAN2[N0])

    def pad_patches(q):
        for i in range(N2):
            padded[i * TOK:i * TOK + TOKENS, :] = pin[N2 * q + i].astype(F32)
        pbuf[pl.ds(aligned(q * N2 * TOK, 16), N2 * TOK), :] = padded[...].astype(BF16)
    for copy in loads:
        copy.wait()
    for item in early:
        forward(item, N1)
    send_own(CHAN1[N1])
    pl.loop(N0, N4)(pad_patches)
    for item in early:
        forward(item, N2)
    send_own(CHAN2[N1])
    send_own(HEAD_W)
    pl.loop(N4, N8)(pad_patches)
    save(pbuf, patch_out)
    forward(CHAN1[N0], N0)
    for item in early:
        finish(item)

    lane32 = lax.broadcasted_iota(jnp.int32, (N1, BAND), N1) // 32

    def lay_out(q, lo, num):
        total = None
        for i in range(N4):
            piece = small[N4 * q + i, lo:lo + num, :]
            piece = jnp.where(lane32 == i, pltpu.roll(piece, 32 * i, N1) if i else piece, 0.0)
            total = piece if total is None else total + piece
        return total
    vec[...] = jnp.zeros(vec.shape, F32)
    rows_first, lnf = ROW_VEC['b_ch1'], ROW_VEC['lnf_g']
    for q in range(N4):
        cols = slice(q * BAND, q * BAND + BAND)
        found = lay_out(q, N0, 16)
        vec[:rows_first, cols] = found[:rows_first]
        vec[lnf:lnf + N2, cols] = found[rows_first:rows_first + N2]
        for layer in range(N2):
            for j in range(N4):
                at = rows_first + N4 * layer + j
                vec[at:at + N1, cols] = small[N4 * j + q, AT_B1 + layer:AT_B1 + layer + N1, :]
        for z in range(N2):
            at = ROW_VEC['b_head'] + z
            vec[at:at + N1, cols] = small[N8 * z, AT_BH + q:AT_BH + q + N1, :]
    for q in range(N2):
        cols = slice(q * BAND, q * BAND + BAND)
        turned = lay_out(q, AT_B1, N8).T
        for layer in range(N2):
            column = AT_BT - AT_B1 + layer
            bt[layer, cols, :] = turned[:, column:column + N1]
            found = lay_out(q, AT_T1 + TOK * layer, TOK)
            t1[layer, :, cols] = found.astype(BF16)
            t1t[layer, cols, :] = found.T.astype(BF16)
            rows = jnp.concatenate([small[N4 * q + i, AT_T2 + 32 * layer:AT_T2 + 32 * layer + 32, :] for i in range(N4)],
                                   axis=N0)
            t2[layer, cols, :] = rows[:, :TOK].astype(BF16)
            t2t[layer, :, cols] = rows.T[:TOK].astype(BF16)

    def vector(name, at=N0):
        return vec[pl.ds(ROW_VEC[name] + at, N1), :]

    tasks = [lambda: forward(CHAN2[N0], N0), lambda: forward(CHAN1[N0], N1)]

    @pl.loop(N0, N2)
    def _(h):
        rows = pl.ds(aligned(h * HALF, HALF), HALF)
        xs[N0][rows, :] = times(pbuf[rows, :], stem_w[...]) + vector('b_stem')
        for k, task in enumerate(tasks):
            pl.when(h == k)(task)
    save(xs[N0], xa_out.at[N0])

    def token_mix(layer, tasks):
        source, target = xs[N2 * layer], xs[N2 * layer + N1]
        gain, shift = vector('ln1_g', layer), vector('ln1_b', layer)

        @pl.loop(N0, IMAGES)
        def _(b):
            rows = pl.ds(aligned(b * TOK, N8), TOK)
            here = source[rows, :]
            norm = (standardize(here)[N0] * gain + shift).astype(BF16)
            hidden = jax.nn.gelu(times(t1t[layer], norm) + bt[layer]).astype(BF16)
            target[rows, :] = here + times(t2t[layer], hidden)
            for k, task in tasks:
                pl.when(b == k)(task)

    def channel_mix(layer, tasks):
        source, target = xs[N2 * layer + N1], xs[N2 * layer + N2]
        gain, shift = vector('ln2_g', layer), vector('ln2_b', layer)

        @pl.loop(N0, BANDS)
        def _(i):
            rows = pl.ds(aligned(i * BAND, BAND), BAND)
            here = source[rows, :]
            v[rows, :] = (standardize(here)[N0] * gain + shift).astype(BF16)
            target[rows, :] = here + vector('b_ch2', layer)

        @pl.loop(N0, N4)
        def _(j):
            cols = pl.ds(aligned(j * WIDE, WIDE), WIDE)
            bias = vector('b_ch1', N4 * layer + j)
            for half in range(N2):
                rows = pl.ds(half * HALF, HALF)
                pre[...] = times(v[rows, :], w1[layer, :, cols])

                @pl.loop(N0, HALF // 32)
                def _(i):
                    part = pl.ds(aligned(i * 32, 32), 32)
                    act[part, :] = jax.nn.gelu(pre[part, :] + bias).astype(BF16)
                target[rows, :] = target[rows, :] + times(act[...], w2[layer, cols, :])
            for k, task in tasks:
                pl.when(j == k)(task)

    token_mix(N0, [(N1, lambda: forward(CHAN2[N0], N1)), (N4, lambda: forward(CHAN1[N0], N2)),
                  (N6, lambda: forward(CHAN2[N0], N2)), (N8, lambda: forward(CHAN1[N1], N0)),
                  (10, lambda: forward(CHAN2[N1], N0)), (12, lambda: forward(HEAD_W, N0)),
                  (14, lambda: forward(CHAN1[N1], N1))])
    save(xs[N1], xb_out.at[N0])
    finish(CHAN1[N0])
    finish(CHAN2[N0])
    save(w1.at[N0], w1_out.at[N0])
    save(w2.at[N0], w2_out.at[N0])
    channel_mix(N0, [(N0, lambda: forward(CHAN2[N1], N1)), (N1, lambda: forward(HEAD_W, N1)),
                    (N2, lambda: forward(CHAN1[N1], N2)), (N3, lambda: forward(CHAN2[N1], N2))])
    save(xs[N2], xa_out.at[N1])
    token_mix(N1, [(N0, lambda: forward(HEAD_W, N2))])
    save(xs[N3], xb_out.at[N1])
    for item in (CHAN1[N1], CHAN2[N1], HEAD_W):
        finish(item)
    save(w1.at[N1], w1_out.at[N1])
    save(w2.at[N1], w2_out.at[N1])
    channel_mix(N1, [])

    real_row = lax.broadcasted_iota(jnp.int32, (TOK, N1), N0) < TOKENS

    @pl.loop(N0, IMAGES)
    def _(b):
        here = xs[N4][pl.ds(aligned(b * TOK, N8), TOK), :]
        pooled[pl.ds(b, N1), :] = row_sum(jnp.where(real_row, here, 0.0)) * (1.0 / TOKENS)
    gain = vector('lnf_g')
    standard, inv_std = standardize(pooled[...])
    norm = standard * gain + vector('lnf_b')
    norm_bf = norm.astype(BF16)
    lane = lax.broadcasted_iota(jnp.int32, (IMAGES, WIDE), N1)
    real = lane < CLASSES_HALF
    logits = [times(norm_bf, head_w[:, z * WIDE:z * WIDE + WIDE]) + vector('b_head', z) for z in range(N2)]
    row_max = jnp.maximum(*[jnp.max(jnp.where(real, l, -jnp.inf), axis=N1, keepdims=True) for l in logits])
    exps = [jnp.where(real, jnp.exp(jnp.where(real, l, row_max) - row_max), 0.0) for l in logits]
    sums = jnp.sum(exps[N0], axis=N1, keepdims=True) + jnp.sum(exps[N1], axis=N1, keepdims=True)
    mine = labels[pl.ds(aligned(tp * IMAGES, N8), IMAGES), :]
    hits = [jnp.logical_and(lane + z * CLASSES_HALF == mine, real) for z in range(N2)]
    picked = sum(jnp.sum(jnp.where(hit, l, 0.0), axis=N1, keepdims=True) for hit, l in zip(hits, logits))
    losses = row_max + jnp.log(sums) - picked
    hs[...] = jnp.zeros(hs.shape, F32)
    turned = norm.T.astype(BF16)
    back = None
    for z in range(N2):
        d_logits = (exps[z] / sums - hits[z].astype(F32)) * (1.0 / TOTAL)
        d_logits_bf = d_logits.astype(BF16)
        gh[:, z * WIDE:z * WIDE + WIDE] = times(turned, d_logits_bf)
        at = ROW_VEC['b_head'] + z
        hs[at:at + N1, :] = row_sum(d_logits)
        piece = by_rows(d_logits_bf, head_w[:, z * WIDE:z * WIDE + WIDE])
        back = piece if back is None else back + piece
    hs[lnf:lnf + N1, :] = row_sum(back * standard)
    hs[lnf + N1:lnf + N2, :] = row_sum(back)
    at = ROW_VEC['loss']
    hs[at:at + N1, :] = jnp.broadcast_to(row_sum(losses) * (1.0 / TOTAL), (N1, WIDE))
    d0[...] = norm_back(back, gain, standard, inv_std) * (1.0 / TOKENS)

    for k, (src, dst) in enumerate(saves):
        pltpu.make_async_copy(src, dst, save_sem.at[k]).wait()
    for item in range(GATHERED):
        for part in DIMS:
            lo, num = GATHER_SPLITS[item][part]
            here = own[item].at[pl.ds(lo, num), :]
            for _ in range(15):
                pltpu.make_async_remote_copy(src_ref=here, dst_ref=here, send_sem=send_sem,
                                             recv_sem=recv_sem.at[item, part, N0], device_id=device_of(coords, core),
                                             device_id_type=MESH).wait_send()


def forward_all(*operands):
    any_spec, vmem = pl.BlockSpec(memory_space=pl.ANY), pl.BlockSpec(memory_space=pltpu.VMEM)
    shape = jax.ShapeDtypeStruct
    plane = (ROWS, WIDE)
    outs = [shape((N2, WIDE, DEEP), BF16), shape((N2, DEEP, WIDE), BF16), shape((N2,) + plane, F32),
            shape((N2,) + plane, F32), shape((ROWS, PATCH), BF16), shape((N2, 256, TOK), BF16),
            shape((N2, TOK, 256), BF16), shape((N2, 256, TOK), BF16), shape((N2, 256, N1), F32),
            shape((VEC_ROWS, WIDE), F32), shape((WIDE, N2 * WIDE), F32), shape((VEC_ROWS, WIDE), F32),
            shape((IMAGES, WIDE), F32)]
    dma = pltpu.SemaphoreType.DMA
    return pl.pallas_call(
        forward_kernel, out_shape=outs, in_specs=[any_spec] + [vmem] * (len(operands) - N1),
        out_specs=[any_spec] * N5 + [vmem] * N8,
        scratch_shapes=[
            pltpu.VMEM((384, 256), BF16), pltpu.VMEM((N2, 64, 1024), BF16), pltpu.VMEM((N2, 128, WIDE), BF16),
            pltpu.VMEM((64, WIDE), BF16), pltpu.VMEM((PACK_ROWS, BAND), F32),
            pltpu.VMEM((PATCH, WIDE), BF16), pltpu.VMEM((16, PACK_ROWS, BAND), F32), pltpu.VMEM((N2, WIDE, DEEP), BF16),
            pltpu.VMEM((N2, DEEP, WIDE), BF16), pltpu.VMEM((WIDE, N2 * WIDE), BF16),
            pltpu.VMEM((IMAGES, TOKENS, PATCH), BF16), pltpu.VMEM((N2 * TOK, PATCH), F32), pltpu.VMEM((ROWS, PATCH), BF16),
            pltpu.VMEM((N2, TOK, 256), BF16)] + [pltpu.VMEM(plane, F32)] * N5 + [
            pltpu.VMEM(plane, BF16), pltpu.VMEM((HALF, WIDE), F32), pltpu.VMEM((HALF, WIDE), BF16),
            pltpu.VMEM((IMAGES, WIDE), F32),
            dma, dma((GATHERED, N3, 15)), dma((IMAGES,)), dma((9,))],
        compiler_params=pltpu.CompilerParams(collective_id=N0, has_side_effects=True, vmem_limit_bytes=67043328),
        cost_estimate=pl.CostEstimate(flops=10 ** 9, bytes_accessed=25 * 10 ** N6, transcendentals=N0),
        name='forward')(*operands)


HEAD, CH1, CH2, STEM = N0, (N1, N3), (N2, N4), N5
ITEM_SHAPES = ((64, 512), (64, 1024), (512, 128), (64, 1024), (512, 128), (256, 384))
ITEM_SPLITS = tuple(tuple((lo, hi - lo) for lo, hi in zip((N0,) + cut, cut + (shape[N0],)))
                    for shape, cut in zip(ITEM_SHAPES, ((24, 48), (24, 48), (176, 344), (24, 48), (176, 344), (88, 176))))
ITEMS = len(ITEM_SHAPES)


def backward_kernel(*refs):
    take = iter(refs)

    def grab(count):
        return [next(take) for _ in range(count)]
    w1_hbm, w2_hbm, t1t, t1, t2, bt, vec, xa_hbm, xb_hbm, d0, patch_hbm, gh_hbm, hs = grab(13)
    o_stem, o1, o2, oh, osum, otok = grab(N6)
    mine, peer = grab(ITEMS), grab(ITEMS)
    boxes = [[grab(N3) for _ in DIMS] for _ in range(ITEMS)]
    w1, w2, xa, xb, grad, acc, v, vt, dout, dout_t, pre, dact, act, dpre, g1, g2, pbuf, gs = grab(18)
    tacc1, tacc2, bacc, sbox, tbox = grab(N5)
    send_sem, hop_sem, peer_sem, pair_sem, load_sem, red_send, red_recv = grab(N7)
    coords, core = my_position()
    other = N1 - core
    entry_barrier(coords, core)
    partner = device_of(coords, other)
    pending = []

    def start(src, dst, sem, device, sent=None):
        copy = pltpu.make_async_remote_copy(src_ref=src, dst_ref=dst, send_sem=send_sem if sent is None else sent,
                                            recv_sem=sem, device_id=device, device_id_type=MESH)
        copy.start()
        return copy

    def arrived(dst, sem):
        pltpu.make_async_remote_copy(src_ref=dst, dst_ref=dst, send_sem=send_sem, recv_sem=sem,
                                     device_id=partner, device_id_type=MESH).wait_recv()

    def left(src, sent):
        pltpu.make_async_remote_copy(src_ref=src, dst_ref=src, send_sem=sent, recv_sem=pair_sem.at[N0],
                                     device_id=partner, device_id_type=MESH).wait_send()

    def view(ref, item, part, select):
        lo, num = ITEM_SPLITS[item][part]
        x, y, z = select
        return ref.at[z, y, x, pl.ds(lo, num), :]

    def phase_source(item, part, phase):
        order = ORDERS[part]
        select = [pl.ds(N0, N2)] * N3
        for dim in order[:phase]:
            select[dim] = coords[dim]
        select[order[phase]] = N1 - coords[order[phase]]
        return view(mine[item], item, part, select)

    def phase_send(item, phase):
        for part in DIMS:
            start(phase_source(item, part, phase), boxes[item][part][phase], hop_sem.at[item, part, phase],
                  device_of(shifted(coords, unit(ORDERS[part][phase])), core))

    def phase_take(item, phase, final=None):
        for part in DIMS:
            order = ORDERS[part]
            box = boxes[item][part][phase]
            arrived(box, hop_sem.at[item, part, phase])
            rest = [dim for dim in (N2, N1, N0) if dim in order[phase + N1:]]
            for sub in range(N2 ** len(rest)):
                bits = [(sub >> place) % N2 for place in range(len(rest))]
                select = list(coords)
                for dim, bit in zip(rest, bits):
                    select[dim] = bit
                here = view(mine[item], item, part, select)
                total = here[...] + (box.at[tuple(bits)] if bits else box)[...]
                if final is None:
                    here[...] = total
                else:
                    lo, num = ITEM_SPLITS[item][part]
                    final[pl.ds(lo, num), :] = total

    def add_peer(item):
        @pl.loop(N0, N8)
        def _(i):
            at = (i // N4, odd(i // N2), odd(i))
            mine[item][at] = mine[item][at] + peer[item][at]

    def advance(items, phase, finals=None):
        for index, item in enumerate(items):
            phase_take(item, phase, None if finals is None else finals[index])
            if phase < N2:
                phase_send(item, phase + N1)

    def reduce_send(parts, stage):
        device = partner if stage == N0 else device_of(shifted(coords, unit(stage - N1)), core)
        for ref, box, slot in parts:
            start(ref, box.at[stage], red_recv.at[slot, stage], device, red_send.at[slot])

    def reduce_take(parts, stage):
        for ref, box, slot in parts:
            arrived(box.at[stage], red_recv.at[slot, stage])
            left(ref, red_send.at[slot])
            ref[...] = ref[...] + box[stage]

    def reduce_step(parts, stage):
        reduce_take(parts, stage)
        if stage < N3:
            reduce_send(parts, stage + N1)

    def load(src, dst, slot):
        copy = pltpu.make_async_copy(src, dst, load_sem.at[slot])
        copy.start()
        return copy

    def head_view(f):
        return gh_hbm.at[pl.ds(aligned(f * 64, 64), 64), :]
    first = [load(w1_hbm.at[N1], w1, N0), load(w2_hbm.at[N1], w2, N1), load(xb_hbm.at[N1], xb, N2)]
    xa_copy = load(xa_hbm.at[N1], xa, N4)
    heads = []
    for y in range(N2):
        for x in range(N2):
            for z in range(N2):
                slot = y * N4 + x * N2 + z
                pending.append(start(head_view(y * N4 + x * N2 + other).at[:, pl.ds(z * WIDE, WIDE)],
                                     peer[HEAD].at[z, y, x], pair_sem.at[slot], partner))
                heads.append(load(head_view(y * N4 + x * N2 + core).at[:, pl.ds(z * WIDE, WIDE)],
                                  mine[HEAD].at[z, y, x], N5 + slot))
    osum[...] = hs[...]
    real_row = lax.broadcasted_iota(jnp.int32, (TOK, N1), N0) < TOKENS

    @pl.loop(N0, IMAGES)
    def _(b):
        grad[pl.ds(aligned(b * TOK, N8), TOK), :] = jnp.where(real_row, d0[pl.ds(b, N1), :], 0.0)

    def head_start():
        for y in range(N2):
            for x in range(N2):
                for z in range(N2):
                    slot = y * N4 + x * N2 + z
                    heads[slot].wait()
                    arrived(peer[HEAD].at[z, y, x], pair_sem.at[slot])
        add_peer(HEAD)
        phase_send(HEAD, N0)

    def add_row(name, at, values):
        row = pl.ds(ROW_VEC[name] + at, N1)
        osum[row, :] = osum[row, :] + values

    def chunk_moves(layer, j):
        z, y = j // N2, odd(j)
        moves = [(g1.at[:, :, other], peer[CH1[layer]].at[z, :, :, :, pl.ds(aligned(y * WIDE, WIDE), WIDE)])]
        for x in range(N2):
            moves.append((g2.at[:, pl.ds(aligned((N2 * x + other) * BAND, BAND), BAND)],
                          peer[CH2[layer]].at[z, y, x]))
        return [(src, dst, peer_sem.at[layer, k, j]) for k, (src, dst) in enumerate(moves)]

    def channel_back(layer, steps):
        gain, shift = vec[pl.ds(ROW_VEC['ln2_g'] + layer, N1), :], vec[pl.ds(ROW_VEC['ln2_b'] + layer, N1), :]

        @pl.loop(N0, BANDS)
        def _(i):
            rows = pl.ds(aligned(i * BAND, BAND), BAND)
            standard, _ = standardize(xb[rows, :])
            norm = standard * gain + shift
            v[rows, :] = norm.astype(BF16)
            vt[:, rows] = norm.T.astype(BF16)
            here = grad[rows, :]
            dout[rows, :] = here.astype(BF16)
            dout_t[:, rows] = here.T.astype(BF16)
            add_row('b_ch2', layer, row_sum(here))
            acc[rows, :] = jnp.zeros((BAND, WIDE), F32)

        @pl.loop(N0, N4)
        def _(j):
            cols = pl.ds(aligned(j * WIDE, WIDE), WIDE)
            bias = vec[pl.ds(ROW_VEC['b_ch1'] + N4 * layer + j, N1), :]
            bacc[...] = jnp.zeros(bacc.shape, F32)
            for half in range(N2):
                rows = pl.ds(half * HALF, HALF)
                pre[...] = times(v[rows, :], w1[:, cols])
                dact[...] = by_rows(dout[rows, :], w2[cols, :])

                @pl.loop(N0, HALF // 32)
                def _(i):
                    small = pl.ds(aligned(i * 32, 32), 32)
                    value, slope = gelu_pair(pre[small, :] + bias)
                    change = dact[small, :] * slope
                    where = pl.ds(aligned(half * HALF + i * 32, 32), 32)
                    act[where, :] = value.astype(BF16)
                    dpre[where, :] = change.astype(BF16)
                    bacc[...] = bacc[...] + jnp.sum(change.reshape(N4, N8, WIDE), axis=N0)
                acc[rows, :] = acc[rows, :] + by_rows(dpre[rows, :], w1[:, cols])
            add_row('b_ch1', N4 * layer + j, row_sum(bacc[...]))

            @pl.when(j > N0)
            def _():
                for src, _, _ in chunk_moves(layer, j):
                    left(src, pair_sem.at[N8])
            g1[...] = times(vt[...], dpre[...]).reshape(g1.shape)
            g2[...] = times(dout_t[...], act[...])
            for src, dst, sem in chunk_moves(layer, j):
                start(src, dst, sem, partner, pair_sem.at[N8])
            z, y = j // N2, odd(j)
            mine[CH1[layer]][z, :, :, :, pl.ds(aligned(y * WIDE, WIDE), WIDE)] = g1[:, :, core]
            for x in range(N2):
                mine[CH2[layer]][z, y, x] = g2[:, pl.ds(aligned((N2 * x + core) * BAND, BAND), BAND)]
            for k, step in enumerate(steps):
                pl.when(j == k)(step)
        for src, _, _ in chunk_moves(layer, N3):
            left(src, pair_sem.at[N8])
        for j in range(N4):
            for _, dst, sem in chunk_moves(layer, j):
                arrived(dst, sem)
        for item in (CH1[layer], CH2[layer]):
            add_peer(item)
            phase_send(item, N0)

        @pl.loop(N0, BANDS)
        def _(i):
            rows = pl.ds(aligned(i * BAND, BAND), BAND)
            standard, inv_std = standardize(xb[rows, :])
            here = acc[rows, :]
            add_row('ln2_g', layer, row_sum(here * standard))
            add_row('ln2_b', layer, row_sum(here))
            grad[rows, :] = grad[rows, :] + norm_back(here, gain, standard, inv_std)

    def token_back(layer, steps):
        gain, shift = vec[pl.ds(ROW_VEC['ln1_g'] + layer, N1), :], vec[pl.ds(ROW_VEC['ln1_b'] + layer, N1), :]
        tacc1[...] = jnp.zeros(tacc1.shape, F32)
        tacc2[...] = jnp.zeros(tacc2.shape, F32)
        pre256, change256 = pre.at[pl.ds(N0, 256), :], dact.at[pl.ds(N0, 256), :]

        @pl.loop(N0, IMAGES)
        def _(b):
            rows = pl.ds(aligned(b * TOK, N8), TOK)
            standard, inv_std = standardize(xa[rows, :])
            norm = (standard * gain + shift).astype(BF16)
            here = grad[rows, :]
            here_bf = here.astype(BF16)
            value, slope = gelu_pair(times(t1t[layer], norm) + bt[layer])
            change = times(t2[layer], here_bf) * slope
            change_bf = change.astype(BF16)
            total = change[:, :BAND]
            for k in range(N1, N4):
                total = total + change[:, k * BAND:(k + N1) * BAND]
            tacc1[:, BAND:] = tacc1[:, BAND:] + total
            tacc1[:, :TOK] = tacc1[:, :TOK] + by_rows(change_bf, norm)
            tacc2[:, :TOK] = tacc2[:, :TOK] + by_rows(value.astype(BF16), here_bf)
            d_norm = times(t1[layer], change_bf)
            add_row('ln1_g', layer, row_sum(d_norm * standard))
            add_row('ln1_b', layer, row_sum(d_norm))
            grad[rows, :] = here + norm_back(d_norm, gain, standard, inv_std)
            for k, step in steps:
                pl.when(b == k)(step)
        lane = lax.broadcasted_iota(jnp.int32, (256, BAND), N1)
        bias_grad = jnp.sum(tacc1[:, BAND:], axis=N1, keepdims=True)
        otok[layer] = (jnp.where(lane < TOK, tacc1[:, :BAND], 0.0)
                       + pltpu.roll(jnp.where(lane < TOK, tacc2[...], 0.0), 64, N1)
                       + jnp.where(lane == BAND - N8, bias_grad, 0.0))

    late = [(otok.at[N1], tbox.at[N1], N1)]
    final = [(otok.at[N0], tbox.at[N0], N0), (osum, sbox, N2)]
    layer1, layer0 = (CH1[N1], CH2[N1]), (CH1[N0], CH2[N0])

    for copy in first:
        copy.wait()
    channel_back(N1, [head_start, lambda: advance([HEAD], N0), lambda: advance([HEAD], N1),
                     lambda: advance([HEAD], N2, [oh])])
    again = [load(w1_hbm.at[N0], w1, N0), load(w2_hbm.at[N0], w2, N1), load(xb_hbm.at[N0], xb, N2)]
    xa_copy.wait()
    token_back(N1, [(11, lambda: advance(layer1, N0))])
    reduce_send(late, N0)
    xa_copy = load(xa_hbm.at[N0], xa, N4)
    for copy in again:
        copy.wait()

    def second():
        advance(layer1, N1)
        reduce_step(late, N1)

    def third():
        advance(layer1, N2, [o1.at[N1], o2.at[N1]])
        reduce_step(late, N2)
    channel_back(N0, [lambda: reduce_step(late, N0), second, third, lambda: reduce_step(late, N3)])
    xa_copy.wait()
    token_back(N0, [(11, lambda: advance(layer0, N0))])

    @pl.loop(N0, BANDS)
    def _(i):
        rows = pl.ds(aligned(i * BAND, BAND), BAND)
        here = grad[rows, :]
        dout_t[:, rows] = here.T.astype(BF16)
        add_row('b_stem', N0, row_sum(here))
    reduce_send(final, N0)

    def patch_load(k):
        f = (k % N4) * N2 + (other if k < N4 else core)
        return load(patch_hbm.at[:, pl.ds(aligned(f * 384, BAND), 384)], pbuf.at[k % N2], k % N2)
    copies = {N0: patch_load(N0)}
    for k in range(N8):
        if k < N7:
            copies[k + N1] = patch_load(k + N1)
        copies[k].wait()
        y, x = (k % N4) // N2, k % N2
        result = times(dout_t[...], pbuf[k % N2]).reshape(N2, 256, 384)
        if k < N4:
            if k > N0:
                left(gs, pair_sem.at[N8])
            gs[...] = result
            start(gs, peer[STEM].at[:, y, x], pair_sem.at[k], partner, pair_sem.at[N8])
        else:
            mine[STEM][:, y, x] = result
        if k == N3:
            left(gs, pair_sem.at[N8])
            reduce_step(final, N0)
        if k == N5:
            advance(layer0, N1)
    for k in range(N4):
        arrived(peer[STEM].at[:, k // N2, k % N2], pair_sem.at[k])
    add_peer(STEM)
    phase_send(STEM, N0)
    reduce_step(final, N1)
    advance(layer0, N2, [o1.at[N0], o2.at[N0]])
    reduce_step(final, N2)
    advance([STEM], N0)
    reduce_step(final, N3)
    advance([STEM], N1)
    advance([STEM], N2, [o_stem])
    for copy in pending:
        copy.wait_send()
    for item in range(ITEMS):
        for part in DIMS:
            for phase in DIMS:
                left(phase_source(item, part, phase), send_sem)


def backward_all(*operands):
    any_spec, vmem = pl.BlockSpec(memory_space=pl.ANY), pl.BlockSpec(memory_space=pltpu.VMEM)
    boxes = [pltpu.VMEM((N2,) * (N2 - phase) + (ITEM_SPLITS[item][part][N1], ITEM_SHAPES[item][N1]), F32)
             for item in range(ITEMS) for part in DIMS for phase in DIMS]
    slots = [pltpu.VMEM((N2, N2, N2) + shape, F32) for shape in ITEM_SHAPES]
    plane = pltpu.VMEM((ROWS, WIDE), F32)
    plane_bf, turned_bf = pltpu.VMEM((ROWS, WIDE), BF16), pltpu.VMEM((WIDE, ROWS), BF16)
    half = pltpu.VMEM((HALF, WIDE), F32)
    dma = pltpu.SemaphoreType.DMA
    outs = ((256, 384), (N2, 64, 1024), (N2, 512, 128), (64, 512), (VEC_ROWS, WIDE), (N2, 256, 128))
    return pl.pallas_call(
        backward_kernel, out_shape=[jax.ShapeDtypeStruct(s, F32) for s in outs],
        in_specs=[any_spec] * N2 + [vmem] * N5 + [any_spec] * N2 + [vmem] + [any_spec] * N2 + [vmem], out_specs=[vmem] * len(outs),
        scratch_shapes=slots + slots + boxes + [
            pltpu.VMEM((WIDE, DEEP), BF16), pltpu.VMEM((DEEP, WIDE), BF16), plane, plane, plane, plane,
            plane_bf, turned_bf, plane_bf, turned_bf, half, half, plane_bf, plane_bf,
            pltpu.VMEM((N2, N2, N2, 64, WIDE), F32), pltpu.VMEM((WIDE, WIDE), F32),
            pltpu.VMEM((N2, ROWS, 384), BF16), pltpu.VMEM((N2, 256, 384), F32),
            pltpu.VMEM((256, 256), F32), pltpu.VMEM((256, 128), F32), pltpu.VMEM((N8, WIDE), F32),
            pltpu.VMEM((N4, VEC_ROWS, WIDE), F32), pltpu.VMEM((N2, N4, 256, 128), F32),
            dma, dma((ITEMS, N3, N3)), dma((N2, N3, N4)), dma((9,)), dma((13,)), dma((N3,)), dma((N3, N4))],
        compiler_params=pltpu.CompilerParams(collective_id=N1, has_side_effects=True, vmem_limit_bytes=67043328),
        cost_estimate=pl.CostEstimate(flops=10 ** 9, bytes_accessed=50 * 10 ** N6, transcendentals=N0),
        name='backward')(*operands)


def weight_specs():
    vec_spec = P(CHANNEL_AXES)
    layer_vec = P(None, CHANNEL_AXES)
    return (P('fsdp', 'tp'), vec_spec, layer_vec, layer_vec, P(None, None, 'fsdp'), P(None, 'fsdp'),
            P(None, 'fsdp', None), layer_vec, layer_vec, P(None, 'fsdp', 'tp'), layer_vec,
            P(None, CHANNEL_AXES, None), layer_vec, vec_spec, vec_spec, P('fsdp', 'tp'), P('tp'))


def solution(mesh):
    def step(patches, labels, w_stem, b_stem, ln1_g, ln1_b, w_tok1, b_tok1, w_tok2,
             ln2_g, ln2_b, w_ch1, b_ch1, w_ch2, b_ch2, lnf_g, lnf_b, w_head, b_head):
        def flat(values):
            return values.reshape(N1, -N1)
        tp, fsdp = lax.axis_index('tp'), lax.axis_index('fsdp')
        w1, w2, xa, xb, padded, t1t, t1, t2, bt, vec, gh, hs, d0 = forward_all(
            patches, labels.reshape(-N1, N1), w_stem, w_ch1, w_ch2, w_head, flat(b_stem), ln1_g, ln1_b, ln2_g, ln2_b,
            b_ch2, flat(lnf_g), flat(lnf_b), b_ch1, b_tok1, flat(b_head), w_tok1, w_tok2)
        o_stem, o1, o2, oh, osum, otok = backward_all(w1, w2, t1t, t1, t2, bt, vec, xa, xb, d0, padded, gh, hs)
        tokens = TOKENS
        owner = tp * N8 + fsdp
        lanes = lax.dynamic_slice_in_dim(osum, owner * 32, 32, N1)
        found = {name: lanes[ROW_VEC[name]:ROW_VEC[name] + num].reshape((num, 32) if num == N2 else (32,))
                 for name, num in VECTORS}
        deep = osum[ROW_VEC['b_ch1']:ROW_VEC['lnf_g']].reshape(N2, DEEP)
        found['b_ch1'] = lax.dynamic_slice_in_dim(deep, owner * 128, 128, N1)
        found['b_head'] = lax.dynamic_slice_in_dim(osum, ROW_VEC['b_head'] + tp, N1, N0)[N0, :500]
        tok_rows = lax.dynamic_slice_in_dim(otok, fsdp * 32, 32, N1)
        found['w_tok1'] = tok_rows[:, :, :tokens].swapaxes(N1, N2)
        found['w_tok2'] = tok_rows[:, :, 64:64 + tokens]
        found['b_tok1'] = tok_rows[:, :, BAND - N8]
        found['w_ch1'], found['w_ch2'] = o1, o2.swapaxes(N1, N2)
        return tuple([osum[ROW_VEC['loss'], N0], o_stem.T, found['b_stem']] + [found[name] for name in LAYER_NAMES]
                     + [found['lnf_g'], found['lnf_b'], oh[:, :500], found['b_head']])

    specs = weight_specs()
    return jax.shard_map(step, mesh=mesh, in_specs=(P('fsdp', None, None), P('fsdp')) + specs,
                         out_specs=(P(),) + specs, check_vma=False)
```

```python
import functools

import jax
import jax.numpy as jnp
from jax import lax
from jax.experimental import pallas as pl
from jax.experimental.pallas import tpu as pltpu
from jax.sharding import PartitionSpec as P

EPS = 1e-6
CHANNEL_AXES = ('tp', 'fsdp')
LAYER_NAMES = ('ln1_g', 'ln1_b', 'w_tok1', 'b_tok1', 'w_tok2', 'ln2_g', 'ln2_b', 'w_ch1', 'b_ch1', 'w_ch2', 'b_ch2')
N0, N1, N2, N3, N4, N5, N6, N7, N8 = range(9)
MESH = pl.DeviceIdType.MESH
BF16 = jnp.bfloat16
F32 = jnp.float32
ORDERS = ((N0, N1, N2), (N1, N2, N0), (N2, N0, N1))


def my_position():
    tp, fsdp = lax.axis_index('tp'), lax.axis_index('fsdp')
    return (lax.rem(fsdp // N2, N2), fsdp // N4, tp), lax.rem(fsdp, N2)


def aligned(value, size):
    return value if isinstance(value, int) else pl.multiple_of(value, size)


def odd(value):
    return value % N2 if isinstance(value, int) else lax.rem(value, N2)


def shifted(coords, bits):
    return tuple(N1 - c if b else c for c, b in zip(coords, bits))


def owner_of(coords, core):
    x, y, z = coords
    return z, y * N4 + x * N2 + core


def device_of(coords, core):
    tp, fsdp = owner_of(coords, core)
    return {'tp': tp, 'fsdp': fsdp}


def unit(dim):
    return tuple(N1 if d == dim else N0 for d in range(N3))


def plus(a, b):
    return tuple((i + j) % N2 for i, j in zip(a, b))


def entry_barrier(coords, core):
    barrier = pltpu.get_barrier_semaphore()
    for dim in range(N3):
        pl.semaphore_signal(barrier, inc=N1, device_id=device_of(shifted(coords, unit(dim)), core), device_id_type=MESH)
    pl.semaphore_signal(barrier, inc=N1, device_id=device_of(coords, N1 - core), device_id_type=MESH)
    pl.semaphore_wait(barrier, N4)


ROW_VEC = dict(b_stem=N0, ln1_g=N1, ln1_b=N3, ln2_g=N5, ln2_b=N7, b_ch2=9, b_ch1=11, lnf_g=19, lnf_b=20, b_head=21, loss=23)
VEC_ROWS = 24
TOK = 49
IMAGES = 16
ROWS = TOK * IMAGES
BAND = 128
STRIP = 112
STRIPS = ROWS // STRIP
WIDE = 512
DEEP = 2048
GELU_A = 0.7978845608028654
GELU_B = 0.044715


def by_rows(left, right):
    return lax.dot_general(left, right, (((N1,), (N1,)), ((), ())), preferred_element_type=F32)


def times(left, right):
    return jnp.dot(left, right, preferred_element_type=F32)


def gelu_pair(pre):
    square = pre * pre
    tanh = jnp.tanh(pre * (GELU_A + (GELU_A * GELU_B) * square))
    cdf = 0.5 + 0.5 * tanh
    value = pre * cdf
    return value, cdf + value * ((1.0 - tanh) * (GELU_A + (3.0 * GELU_A * GELU_B) * square))


def gelu_value(pre):
    return pre * (0.5 + 0.5 * jnp.tanh(pre * (GELU_A + (GELU_A * GELU_B) * (pre * pre))))


def image_rows(b):
    return pl.ds(b, TOK, stride=IMAGES)


def get(ref, rows):
    return jnp.concatenate([ref[k, rows, :] for k in range(N4)], axis=N1)


def put(ref, rows, values):
    for k in range(N4):
        ref[k, rows, :] = values[:, k * BAND:(k + N1) * BAND]


def strip_rows(i):
    return pl.ds(aligned(i * STRIP, STRIP), STRIP)


def turn(dst, read):
    whole = ROWS // BAND

    @pl.loop(N0, whole)
    def _(i):
        rows = pl.ds(aligned(i * BAND, BAND), BAND)
        dst[:, rows] = read(rows).astype(F32).T.astype(BF16)
    dst[:, whole * BAND:] = read(pl.ds(whole * BAND, ROWS % BAND)).astype(F32).T.astype(BF16)


def standardize(values):
    centered = values - jnp.mean(values, axis=N1, keepdims=True)
    inv_std = lax.rsqrt(jnp.mean(centered * centered, axis=N1, keepdims=True) + EPS)
    return centered * inv_std, inv_std


def norm_back(grad_out, gain, standard, inv_std):
    grad_std = grad_out * gain
    first = jnp.mean(grad_std, axis=N1, keepdims=True)
    second = jnp.mean(grad_std * standard, axis=N1, keepdims=True)
    return inv_std * (grad_std - first - standard * second)


def row_sum(values):
    return jnp.sum(values, axis=N0, keepdims=True)


DIMS = range(N3)


STEM_W, SMALL, HEAD_W, CHAN1, CHAN2 = N0, N1, N6, (N2, N4), (N3, N5)
GATHER_SPLITS = (((N0, 128), (128, 128), (256, 128)), ((N0, 32), (32, 32), (64, 24)),
                 ((N0, 16), (16, 16), (32, 32)), ((N0, 48), (48, 48), (96, 32)),
                 ((N0, 16), (16, 16), (32, 32)), ((N0, 48), (48, 48), (96, 32)), ((N0, 32), (32, 16), (48, 16)))
GATHERED = len(GATHER_SPLITS)
PACK_ROWS = 88
AT_B1, AT_BT, AT_BH, AT_T = 16, 18, 20, 24
VECTORS = (('b_stem', N1), ('ln1_g', N2), ('ln1_b', N2), ('ln2_g', N2), ('ln2_b', N2), ('b_ch2', N2), ('lnf_g', N1), ('lnf_b', N1))
CLASSES_HALF = 500
TOTAL = 256
PATCH = 3072


def forward_kernel(*refs):
    take = iter(refs)

    def grab(count):
        return [next(take) for _ in range(count)]
    patch_hbm, labels, f_stem, f1, f2, f_head = grab(N6)
    vec_in = grab(len(VECTORS))
    i_b1, i_bt, i_bh, i_t1, i_t2 = grab(N5)
    w1_out, w2_out, xa_out, xb_out, t1t, t1, t2, bt, vec, gh, hs, d0 = grab(12)
    own_stem, own1, own2, own_head, pack = grab(N5)
    stem_w, small, w1, w2, head_w = grab(N5)
    pin, t2t = grab(N2)
    xs = grab(N5)
    v, pre, act, pooled = grab(N4)
    send_sem, recv_sem, load_sem, save_sem = grab(N4)
    coords, core = my_position()
    tp = coords[N2]
    patch_copy = pltpu.make_async_copy(patch_hbm.at[:, pl.ds(aligned(tp * IMAGES, IMAGES), IMAGES), :], pin, load_sem)
    patch_copy.start()

    own_stem[...] = f_stem[...].astype(BF16)
    own1[...] = f1[...].astype(BF16)
    own2[...] = f2[...].astype(BF16)
    own_head[...] = jnp.zeros(own_head.shape, BF16)
    own_head[:, :CLASSES_HALF] = f_head[...].astype(BF16)
    pack[...] = jnp.zeros(pack.shape, F32)
    row = N0
    for ref, (_, num) in zip(vec_in, VECTORS):
        pack[row:row + num, :32] = ref[...]
        row += num
    pack[AT_B1:AT_B1 + N2, :] = i_b1[...]
    pack[AT_BT:AT_BT + N2, :32] = i_bt[...]
    for k in range(N4):
        width = min(BAND, CLASSES_HALF - k * BAND)
        pack[AT_BH + k:AT_BH + k + N1, :width] = i_bh[:, k * BAND:k * BAND + width]
    for layer in range(N2):
        at = AT_T + 32 * layer
        pack[at:at + 32, :TOK] = i_t1[layer]
        pack[at:at + 32, 64:64 + TOK] = i_t2[layer]
    entry_barrier(coords, core)

    own = [own_stem, pack, own1.at[N0], own2.at[N0], own1.at[N1], own2.at[N1], own_head]

    def block(item, tp, fsdp, lo, num):
        if item == STEM_W:
            return stem_w.at[pl.ds(aligned(fsdp * 384 + lo, 128), num), pl.ds(aligned(tp * 256, 128), 256)]
        if item == SMALL:
            return small.at[tp * N8 + fsdp, pl.ds(lo, num), :]
        if item in CHAN1:
            return w1.at[CHAN1.index(item), pl.ds(aligned(fsdp * 64 + lo, 16), num), pl.ds(aligned(tp * 1024, 128), 1024)]
        if item in CHAN2:
            return w2.at[CHAN2.index(item), pl.ds(aligned((tp * N8 + fsdp) * 128 + lo, 16), num), :]
        return head_w.at[pl.ds(aligned(fsdp * 64 + lo, 16), num), pl.ds(aligned(tp * WIDE, 128), WIDE)]

    def move(item, part, bits, is_own, target, slot):
        lo, num = GATHER_SPLITS[item][part]
        there = block(item, *owner_of(shifted(coords, bits), core), lo, num)
        here = own[item].at[pl.ds(lo, num), :] if is_own else there
        pltpu.make_async_remote_copy(src_ref=here, dst_ref=there, send_sem=send_sem,
                                     recv_sem=recv_sem.at[item, part, slot], device_id=target,
                                     device_id_type=MESH).start()

    def arrival(item, part, bits, from_core, slot):
        lo, num = GATHER_SPLITS[item][part]
        there = block(item, *owner_of(shifted(coords, bits), from_core), lo, num)
        pltpu.make_async_remote_copy(src_ref=there, dst_ref=there, send_sem=send_sem,
                                     recv_sem=recv_sem.at[item, part, slot], device_id=device_of(coords, core),
                                     device_id_type=MESH).wait_recv()

    def pass_on(item, part, bits, level):
        order = ORDERS[part]
        rank = sum(N2 ** i for i in DIMS if bits[order[i]])
        for step in range(level, N3):
            move(item, part, bits, False, device_of(shifted(coords, unit(order[step])), core), N2 ** step - N1 + rank)
        move(item, part, bits, False, device_of(coords, N1 - core), N7 + rank)

    def bits_of(part, rank):
        bits = [N0, N0, N0]
        for i in DIMS:
            bits[ORDERS[part][i]] = (rank >> i) % N2
        return tuple(bits)

    def send_own(item):
        none = (N0, N0, N0)
        for step in DIMS:
            for part in DIMS:
                target = device_of(shifted(coords, unit(ORDERS[part][step])), core)
                move(item, part, none, True, target, N2 ** step - N1)
        for part in DIMS:
            move(item, part, none, True, device_of(coords, N1 - core), N7)

    def forward(item, level):
        for part in DIMS:
            for rank in range(N2 ** level):
                bits = bits_of(part, rank + N2 ** level)
                arrival(item, part, bits, core, N2 ** level - N1 + rank)
                pass_on(item, part, bits, level + N1)

    def finish(item):
        for part in DIMS:
            for rank in range(N8):
                arrival(item, part, bits_of(part, rank), N1 - core, N7 + rank)

    def place_own(item):
        here = own[item]
        block(item, *owner_of(coords, core), N0, here.shape[N0])[...] = here[...]

    saves = []

    def save(src, dst):
        copy = pltpu.make_async_copy(src, dst, save_sem.at[len(saves)])
        copy.start()
        saves.append((src, dst))

    early = (SMALL, STEM_W)
    for item in early:
        send_own(item)
    for item in range(GATHERED):
        place_own(item)
    for level in range(N2):
        for item in early:
            forward(item, level)
    send_own(CHAN1[N0])
    for item in early:
        forward(item, N2)
    send_own(CHAN2[N0])
    finish(SMALL)

    lane32 = lax.broadcasted_iota(jnp.int32, (N1, BAND), N1) // 32

    def lay_out(q, lo, num):
        total = None
        for i in range(N4):
            piece = small[N4 * q + i, lo:lo + num, :]
            piece = jnp.where(lane32 == i, pltpu.roll(piece, 32 * i, N1) if i else piece, 0.0)
            total = piece if total is None else total + piece
        return total
    vec[...] = jnp.zeros(vec.shape, F32)
    rows_first, lnf = ROW_VEC['b_ch1'], ROW_VEC['lnf_g']
    for q in range(N4):
        cols = slice(q * BAND, q * BAND + BAND)
        found = lay_out(q, N0, 16)
        vec[:rows_first, cols] = found[:rows_first]
        vec[lnf:lnf + N2, cols] = found[rows_first:rows_first + N2]
        for layer in range(N2):
            for j in range(N4):
                at = rows_first + N4 * layer + j
                vec[at:at + N1, cols] = small[N4 * j + q, AT_B1 + layer:AT_B1 + layer + N1, :]
        for z in range(N2):
            at = ROW_VEC['b_head'] + z
            vec[at:at + N1, cols] = small[N8 * z, AT_BH + q:AT_BH + q + N1, :]
    for q in range(N2):
        cols = slice(q * BAND, q * BAND + BAND)
        turned = lay_out(q, AT_B1, N8).T
        for layer in range(N2):
            column = AT_BT - AT_B1 + layer
            bt[layer, cols, :] = turned[:, column:column + N1]
            at = AT_T + 32 * layer
            rows = jnp.concatenate([small[N4 * q + i, at:at + 32, :] for i in range(N4)], axis=N0)
            back = rows.T
            t1t[layer, cols, :] = rows[:, :TOK].astype(BF16)
            t1[layer, :, cols] = back[:TOK].astype(BF16)
            t2[layer, cols, :] = pltpu.roll(rows, 64, N1)[:, :TOK].astype(BF16)
            t2t[layer, :, cols] = back[64:64 + TOK].astype(BF16)

    def vector(name, at=N0):
        return vec[pl.ds(ROW_VEC[name] + at, N1), :]

    forward(CHAN1[N0], N0)
    finish(STEM_W)
    patch_copy.wait()
    cut = TOK // N2 + N1
    for lo, num, tasks in ((N0, cut, ((CHAN2[N0], N0), (CHAN1[N0], N1))), (cut, TOK - cut, ((CHAN2[N0], N1),))):
        rows = pl.ds(lo * IMAGES, num * IMAGES)
        patches = pin[lo:lo + num].reshape(num * IMAGES, PATCH)
        put(xs[N0], rows, times(patches, stem_w[...]) + vector('b_stem'))
        for item, level in tasks:
            forward(item, level)
        send_own(CHAN2[N1] if lo else CHAN1[N1])
    save(xs[N0], xa_out.at[N0])

    def token_mix(layer, tasks):
        source, target = xs[N2 * layer], xs[N2 * layer + N1]
        gain, shift = vector('ln1_g', layer), vector('ln1_b', layer)

        @pl.loop(N0, IMAGES // N2)
        def _(pair):
            rows = [image_rows(N2 * pair + i) for i in range(N2)]
            here = [get(source, r) for r in rows]
            norm = [(standardize(x)[N0] * gain + shift).astype(BF16) for x in here]
            hidden = [gelu_value(times(t1t[layer], n) + bt[layer]).astype(BF16) for n in norm]
            mixed = [x + times(t2t[layer], h) for x, h in zip(here, hidden)]
            for r, x in zip(rows, mixed):
                put(target, r, x)
            for k, task in enumerate(tasks):
                pl.when(pair == k)(task)

    def channel_mix(layer, tasks):
        source, target = xs[N2 * layer + N1], xs[N2 * layer + N2]
        gain, shift = vector('ln2_g', layer), vector('ln2_b', layer)

        @pl.loop(N0, STRIPS)
        def _(i):
            rows = strip_rows(i)
            here = get(source, rows)
            v[rows, :] = (standardize(here)[N0] * gain + shift).astype(BF16)
            put(target, rows, here + vector('b_ch2', layer))

        @pl.loop(N0, N4)
        def _(j):
            cols = pl.ds(aligned(j * WIDE, WIDE), WIDE)
            bias = vector('b_ch1', N4 * layer + j)
            pre[...] = times(v[...], w1[layer, :, cols])

            @pl.loop(N0, STRIPS)
            def _(i):
                rows = strip_rows(i)
                act[rows, :] = gelu_value(pre[rows, :] + bias).astype(BF16)
            everything = pl.ds(N0, ROWS)
            put(target, everything, get(target, everything) + times(act[...], w2[layer, cols, :]))
            for k, task in enumerate(tasks):
                pl.when(j == k)(task)

    def both(first, second):
        def run():
            first()
            second()
        return run

    def step(item, level):
        return lambda: forward(item, level)
    token_mix(N0, [step(CHAN1[N0], N2), step(CHAN2[N0], N2), both(step(CHAN1[N1], N0), lambda: send_own(HEAD_W)),
                  step(CHAN2[N1], N0), step(CHAN1[N1], N1), step(CHAN2[N1], N1), step(HEAD_W, N0), step(CHAN1[N1], N2)])
    save(xs[N1], xb_out.at[N0])
    finish(CHAN1[N0])
    finish(CHAN2[N0])
    save(w1.at[N0], w1_out.at[N0])
    save(w2.at[N0], w2_out.at[N0])
    channel_mix(N0, [step(CHAN2[N1], N2), step(HEAD_W, N1), step(HEAD_W, N2)])
    save(xs[N2], xa_out.at[N1])
    token_mix(N1, [])
    save(xs[N3], xb_out.at[N1])
    for item in (CHAN1[N1], CHAN2[N1], HEAD_W):
        finish(item)
    save(w1.at[N1], w1_out.at[N1])
    save(w2.at[N1], w2_out.at[N1])
    channel_mix(N1, [])

    pooled[...] = jnp.zeros(pooled.shape, F32)

    @pl.loop(N0, TOK)
    def _(t):
        pooled[...] = pooled[...] + get(xs[N4], pl.ds(aligned(t * IMAGES, IMAGES), IMAGES))
    gain = vector('lnf_g')
    standard, inv_std = standardize(pooled[...] * (1.0 / TOK))
    norm = standard * gain + vector('lnf_b')
    norm_bf = norm.astype(BF16)
    lane = lax.broadcasted_iota(jnp.int32, (IMAGES, WIDE), N1)
    real = lane < CLASSES_HALF
    logits = [times(norm_bf, head_w[:, z * WIDE:z * WIDE + WIDE]) + vector('b_head', z) for z in range(N2)]
    row_max = jnp.maximum(*[jnp.max(jnp.where(real, l, -jnp.inf), axis=N1, keepdims=True) for l in logits])
    exps = [jnp.where(real, jnp.exp(jnp.where(real, l, row_max) - row_max), 0.0) for l in logits]
    sums = jnp.sum(exps[N0], axis=N1, keepdims=True) + jnp.sum(exps[N1], axis=N1, keepdims=True)
    mine = labels[pl.ds(aligned(tp * IMAGES, N8), IMAGES), :]
    hits = [jnp.logical_and(lane + z * CLASSES_HALF == mine, real) for z in range(N2)]
    picked = sum(jnp.sum(jnp.where(hit, l, 0.0), axis=N1, keepdims=True) for hit, l in zip(hits, logits))
    losses = row_max + jnp.log(sums) - picked
    hs[...] = jnp.zeros(hs.shape, F32)
    turned = norm.T.astype(BF16)
    back = None
    for z in range(N2):
        d_logits = (exps[z] / sums - hits[z].astype(F32)) * (1.0 / TOTAL)
        d_logits_bf = d_logits.astype(BF16)
        gh[:, z * WIDE:z * WIDE + WIDE] = times(turned, d_logits_bf)
        at = ROW_VEC['b_head'] + z
        hs[at:at + N1, :] = row_sum(d_logits)
        piece = by_rows(d_logits_bf, head_w[:, z * WIDE:z * WIDE + WIDE])
        back = piece if back is None else back + piece
    hs[lnf:lnf + N1, :] = row_sum(back * standard)
    hs[lnf + N1:lnf + N2, :] = row_sum(back)
    at = ROW_VEC['loss']
    hs[at:at + N1, :] = jnp.broadcast_to(row_sum(losses) * (1.0 / TOTAL), (N1, WIDE))
    d0[...] = norm_back(back, gain, standard, inv_std) * (1.0 / TOK)

    for k, (src, dst) in enumerate(saves):
        pltpu.make_async_copy(src, dst, save_sem.at[k]).wait()
    for item in range(GATHERED):
        for part in DIMS:
            lo, num = GATHER_SPLITS[item][part]
            here = own[item].at[pl.ds(lo, num), :]
            for _ in range(15):
                pltpu.make_async_remote_copy(src_ref=here, dst_ref=here, send_sem=send_sem,
                                             recv_sem=recv_sem.at[item, part, N0], device_id=device_of(coords, core),
                                             device_id_type=MESH).wait_send()


def forward_all(*operands):
    any_spec, vmem = pl.BlockSpec(memory_space=pl.ANY), pl.BlockSpec(memory_space=pltpu.VMEM)
    shape = jax.ShapeDtypeStruct
    plane, blocks = (ROWS, WIDE), (N4, ROWS, BAND)
    outs = [shape((N2, WIDE, DEEP), BF16), shape((N2, DEEP, WIDE), BF16), shape((N2,) + blocks, F32),
            shape((N2,) + blocks, F32), shape((N2, 256, TOK), BF16),
            shape((N2, TOK, 256), BF16), shape((N2, 256, TOK), BF16), shape((N2, 256, N1), F32),
            shape((VEC_ROWS, WIDE), F32), shape((WIDE, N2 * WIDE), F32), shape((VEC_ROWS, WIDE), F32),
            shape((IMAGES, WIDE), F32)]
    dma = pltpu.SemaphoreType.DMA
    return pl.pallas_call(
        forward_kernel, out_shape=outs, in_specs=[any_spec] + [vmem] * (len(operands) - N1),
        out_specs=[any_spec] * N4 + [vmem] * N8,
        scratch_shapes=[
            pltpu.VMEM((384, 256), BF16), pltpu.VMEM((N2, 64, 1024), BF16), pltpu.VMEM((N2, 128, WIDE), BF16),
            pltpu.VMEM((64, WIDE), BF16), pltpu.VMEM((PACK_ROWS, BAND), F32),
            pltpu.VMEM((PATCH, WIDE), BF16), pltpu.VMEM((16, PACK_ROWS, BAND), F32), pltpu.VMEM((N2, WIDE, DEEP), BF16),
            pltpu.VMEM((N2, DEEP, WIDE), BF16), pltpu.VMEM((WIDE, N2 * WIDE), BF16),
            pltpu.VMEM((TOK, IMAGES, PATCH), BF16),
            pltpu.VMEM((N2, TOK, 256), BF16)] + [pltpu.VMEM(blocks, F32)] * N5 + [
            pltpu.VMEM(plane, BF16), pltpu.VMEM(plane, F32), pltpu.VMEM(plane, BF16),
            pltpu.VMEM((IMAGES, WIDE), F32),
            dma, dma((GATHERED, N3, 15)), dma, dma((N8,))],
        compiler_params=pltpu.CompilerParams(collective_id=N0, has_side_effects=True, vmem_limit_bytes=67043328),
        cost_estimate=pl.CostEstimate(flops=10 ** 9, bytes_accessed=25 * 10 ** N6, transcendentals=N0),
        name='forward')(*operands)


HEAD, CH1, CH2, STEM = N0, (N1, N3), (N2, N4), N5
ITEM_SHAPES = ((64, 512), (64, 1024), (512, 128), (64, 1024), (512, 128), (256, 384))
ITEM_SPLITS = tuple(tuple((lo, hi - lo) for lo, hi in zip((N0,) + cut, cut + (shape[N0],)))
                    for shape, cut in zip(ITEM_SHAPES, ((24, 48), (24, 48), (176, 344), (24, 48), (176, 344), (88, 176))))
ITEMS = len(ITEM_SHAPES)


def backward_kernel(*refs):
    take = iter(refs)

    def grab(count):
        return [next(take) for _ in range(count)]
    w1_hbm, w2_hbm, t1t, t1, t2, bt, vec, xa_hbm, xb_hbm, d0, patch_hbm, gh_hbm, hs = grab(13)
    o_stem, o1, o2, oh, osum, otok = grab(N6)
    mine, peer = grab(ITEMS), grab(ITEMS)
    boxes = [[grab(N3) for _ in DIMS] for _ in range(ITEMS)]
    w1, w2, xa, xb, grad, acc, v, vt, dout, dout_t, pre, dact, act, dpre, g1, g2, pbuf = grab(17)
    tacc1, tacc2, bacc, sbox, tbox = grab(N5)
    send_sem, hop_sem, peer_sem, pair_sem, load_sem, red_send, red_recv = grab(N7)
    coords, core = my_position()
    other = N1 - core
    entry_barrier(coords, core)
    partner = device_of(coords, other)
    pending = []

    def start(src, dst, sem, device, sent=None):
        copy = pltpu.make_async_remote_copy(src_ref=src, dst_ref=dst, send_sem=send_sem if sent is None else sent,
                                            recv_sem=sem, device_id=device, device_id_type=MESH)
        copy.start()
        return copy

    def arrived(dst, sem):
        pltpu.make_async_remote_copy(src_ref=dst, dst_ref=dst, send_sem=send_sem, recv_sem=sem,
                                     device_id=partner, device_id_type=MESH).wait_recv()

    def left(src, sent):
        pltpu.make_async_remote_copy(src_ref=src, dst_ref=src, send_sem=sent, recv_sem=pair_sem.at[N0],
                                     device_id=partner, device_id_type=MESH).wait_send()

    def view(ref, item, part, select):
        lo, num = ITEM_SPLITS[item][part]
        x, y, z = select
        return ref.at[z, y, x, pl.ds(lo, num), :]

    def phase_source(item, part, phase):
        order = ORDERS[part]
        select = [pl.ds(N0, N2)] * N3
        for dim in order[:phase]:
            select[dim] = coords[dim]
        select[order[phase]] = N1 - coords[order[phase]]
        return view(mine[item], item, part, select)

    def phase_send(item, phase):
        for part in DIMS:
            start(phase_source(item, part, phase), boxes[item][part][phase], hop_sem.at[item, part, phase],
                  device_of(shifted(coords, unit(ORDERS[part][phase])), core))

    def phase_take(item, phase, final=None):
        for part in DIMS:
            order = ORDERS[part]
            box = boxes[item][part][phase]
            arrived(box, hop_sem.at[item, part, phase])
            rest = [dim for dim in (N2, N1, N0) if dim in order[phase + N1:]]
            for sub in range(N2 ** len(rest)):
                bits = [(sub >> place) % N2 for place in range(len(rest))]
                select = list(coords)
                for dim, bit in zip(rest, bits):
                    select[dim] = bit
                here = view(mine[item], item, part, select)
                total = here[...] + (box.at[tuple(bits)] if bits else box)[...]
                if final is None:
                    here[...] = total
                else:
                    lo, num = ITEM_SPLITS[item][part]
                    final[pl.ds(lo, num), :] = total

    def add_peer(item):
        @pl.loop(N0, N8)
        def _(i):
            at = (i // N4, odd(i // N2), odd(i))
            mine[item][at] = mine[item][at] + peer[item][at]

    def advance(items, phase, finals=None):
        for index, item in enumerate(items):
            phase_take(item, phase, None if finals is None else finals[index])
            if phase < N2:
                phase_send(item, phase + N1)

    def reduce_send(parts, stage):
        device = partner if stage == N0 else device_of(shifted(coords, unit(stage - N1)), core)
        for ref, box, slot in parts:
            start(ref, box.at[stage], red_recv.at[slot, stage], device, red_send.at[slot])

    def reduce_take(parts, stage):
        for ref, box, slot in parts:
            arrived(box.at[stage], red_recv.at[slot, stage])
            left(ref, red_send.at[slot])
            ref[...] = ref[...] + box[stage]

    def reduce_step(parts, stage):
        reduce_take(parts, stage)
        if stage < N3:
            reduce_send(parts, stage + N1)

    def load(src, dst, slot):
        copy = pltpu.make_async_copy(src, dst, load_sem.at[slot])
        copy.start()
        return copy

    def head_view(f):
        return gh_hbm.at[pl.ds(aligned(f * 64, 64), 64), :]
    first = [load(w1_hbm.at[N1], w1, N0), load(w2_hbm.at[N1], w2, N1), load(xb_hbm.at[N1], xb, N2)]
    xa_copy = load(xa_hbm.at[N1], xa, N4)
    heads = []
    for y in range(N2):
        for x in range(N2):
            for z in range(N2):
                slot = y * N4 + x * N2 + z
                pending.append(start(head_view(y * N4 + x * N2 + other).at[:, pl.ds(z * WIDE, WIDE)],
                                     peer[HEAD].at[z, y, x], pair_sem.at[slot], partner))
                heads.append(load(head_view(y * N4 + x * N2 + core).at[:, pl.ds(z * WIDE, WIDE)],
                                  mine[HEAD].at[z, y, x], N5 + slot))
    osum[...] = hs[...]

    @pl.loop(N0, TOK)
    def _(t):
        put(grad, pl.ds(aligned(t * IMAGES, IMAGES), IMAGES), d0[...])

    def head_start():
        for y in range(N2):
            for x in range(N2):
                for z in range(N2):
                    slot = y * N4 + x * N2 + z
                    heads[slot].wait()
                    arrived(peer[HEAD].at[z, y, x], pair_sem.at[slot])
        add_peer(HEAD)
        phase_send(HEAD, N0)

    def add_row(name, at, values):
        row = pl.ds(ROW_VEC[name] + at, N1)
        osum[row, :] = osum[row, :] + values

    def chunk_moves(layer, j):
        z, y = j // N2, odd(j)
        moves = [(g1.at[:, :, other], peer[CH1[layer]].at[z, :, :, :, pl.ds(aligned(y * WIDE, WIDE), WIDE)])]
        for x in range(N2):
            moves.append((g2.at[:, pl.ds(aligned((N2 * x + other) * BAND, BAND), BAND)],
                          peer[CH2[layer]].at[z, y, x]))
        return [(src, dst, peer_sem.at[layer, k, j]) for k, (src, dst) in enumerate(moves)]

    def channel_back(layer, steps):
        gain, shift = vec[pl.ds(ROW_VEC['ln2_g'] + layer, N1), :], vec[pl.ds(ROW_VEC['ln2_b'] + layer, N1), :]

        @pl.loop(N0, STRIPS)
        def _(i):
            rows = strip_rows(i)
            standard, _ = standardize(get(xb, rows))
            v[rows, :] = (standard * gain + shift).astype(BF16)
            here = get(grad, rows)
            dout[rows, :] = here.astype(BF16)
            add_row('b_ch2', layer, row_sum(here))
            acc[rows, :] = jnp.zeros((STRIP, WIDE), F32)
        turn(vt, lambda rows: v[rows, :])
        turn(dout_t, lambda rows: dout[rows, :])

        @pl.loop(N0, N4)
        def _(j):
            cols = pl.ds(aligned(j * WIDE, WIDE), WIDE)
            bias = vec[pl.ds(ROW_VEC['b_ch1'] + N4 * layer + j, N1), :]
            bacc[...] = jnp.zeros(bacc.shape, F32)
            pre[...] = times(v[...], w1[:, cols])
            dact[...] = by_rows(dout[...], w2[cols, :])

            @pl.loop(N0, STRIPS)
            def _(i):
                rows = strip_rows(i)
                value, slope = gelu_pair(pre[rows, :] + bias)
                change = dact[rows, :] * slope
                act[rows, :] = value.astype(BF16)
                dpre[rows, :] = change.astype(BF16)
                bacc[...] = bacc[...] + jnp.sum(change.reshape(STRIP // N8, N8, WIDE), axis=N0)
            acc[...] = acc[...] + by_rows(dpre[...], w1[:, cols])
            add_row('b_ch1', N4 * layer + j, row_sum(bacc[...]))

            @pl.when(j > N0)
            def _():
                for src, _, _ in chunk_moves(layer, j):
                    left(src, pair_sem.at[N8])
            g1[...] = times(vt[...], dpre[...]).reshape(g1.shape)
            g2[...] = times(dout_t[...], act[...])
            for src, dst, sem in chunk_moves(layer, j):
                start(src, dst, sem, partner, pair_sem.at[N8])
            z, y = j // N2, odd(j)
            mine[CH1[layer]][z, :, :, :, pl.ds(aligned(y * WIDE, WIDE), WIDE)] = g1[:, :, core]
            for x in range(N2):
                mine[CH2[layer]][z, y, x] = g2[:, pl.ds(aligned((N2 * x + core) * BAND, BAND), BAND)]
            for k, step in enumerate(steps):
                pl.when(j == k)(step)
        for src, _, _ in chunk_moves(layer, N3):
            left(src, pair_sem.at[N8])
        for j in range(N4):
            for _, dst, sem in chunk_moves(layer, j):
                arrived(dst, sem)
        for item in (CH1[layer], CH2[layer]):
            add_peer(item)
            phase_send(item, N0)

        @pl.loop(N0, STRIPS)
        def _(i):
            rows = strip_rows(i)
            standard, inv_std = standardize(get(xb, rows))
            here = acc[rows, :]
            add_row('ln2_g', layer, row_sum(here * standard))
            add_row('ln2_b', layer, row_sum(here))
            put(grad, rows, get(grad, rows) + norm_back(here, gain, standard, inv_std))

    def token_back(layer, steps):
        gain, shift = vec[pl.ds(ROW_VEC['ln1_g'] + layer, N1), :], vec[pl.ds(ROW_VEC['ln1_b'] + layer, N1), :]
        tacc1[...] = jnp.zeros(tacc1.shape, F32)
        tacc2[...] = jnp.zeros(tacc2.shape, F32)

        @pl.loop(N0, IMAGES // N2)
        def _(pair):
            rows = [image_rows(N2 * pair + i) for i in range(N2)]
            both = range(len(rows))
            inputs, heres = [get(xa, r) for r in rows], [get(grad, r) for r in rows]
            standards, invs = zip(*[standardize(x) for x in inputs])
            norms = [(x * gain + shift).astype(BF16) for x in standards]
            heres_bf = [x.astype(BF16) for x in heres]
            values, slopes = zip(*[gelu_pair(times(t1t[layer], x) + bt[layer]) for x in norms])
            changes = [times(t2[layer], x) * slope for x, slope in zip(heres_bf, slopes)]
            changes_bf = [x.astype(BF16) for x in changes]
            total = sum(x[:, k * BAND:(k + N1) * BAND] for x in changes for k in range(N4))
            d_norms = [times(t1[layer], x) for x in changes_bf]
            tacc1[:, BAND:] = tacc1[:, BAND:] + total
            tacc1[:, :TOK] = tacc1[:, :TOK] + sum(by_rows(changes_bf[i], norms[i]) for i in both)
            tacc2[:, :TOK] = tacc2[:, :TOK] + sum(by_rows(values[i].astype(BF16), heres_bf[i]) for i in both)
            add_row('ln1_g', layer, sum(row_sum(d_norms[i] * standards[i]) for i in both))
            add_row('ln1_b', layer, sum(row_sum(d_norms[i]) for i in both))
            results = [heres[i] + norm_back(d_norms[i], gain, standards[i], invs[i]) for i in both]
            for r, x in zip(rows, results):
                put(grad, r, x)
            for k, step in steps:
                pl.when(pair == k)(step)
        lane = lax.broadcasted_iota(jnp.int32, (256, BAND), N1)
        bias_grad = jnp.sum(tacc1[:, BAND:], axis=N1, keepdims=True)
        otok[layer] = (jnp.where(lane < TOK, tacc1[:, :BAND], 0.0)
                       + pltpu.roll(jnp.where(lane < TOK, tacc2[...], 0.0), 64, N1)
                       + jnp.where(lane == BAND - N8, bias_grad, 0.0))

    late = [(otok.at[N1], tbox.at[N1], N1)]
    final = [(otok.at[N0], tbox.at[N0], N0), (osum, sbox, N2)]
    layer1, layer0 = (CH1[N1], CH2[N1]), (CH1[N0], CH2[N0])

    for copy in first:
        copy.wait()
    channel_back(N1, [head_start, lambda: advance([HEAD], N0), lambda: advance([HEAD], N1),
                     lambda: advance([HEAD], N2, [oh])])
    again = [load(w1_hbm.at[N0], w1, N0), load(w2_hbm.at[N0], w2, N1), load(xb_hbm.at[N0], xb, N2)]
    xa_copy.wait()
    token_back(N1, [(N5, lambda: advance(layer1, N0))])
    reduce_send(late, N0)
    xa_copy = load(xa_hbm.at[N0], xa, N4)
    for copy in again:
        copy.wait()

    def second():
        advance(layer1, N1)
        reduce_step(late, N1)

    def third():
        advance(layer1, N2, [o1.at[N1], o2.at[N1]])
        reduce_step(late, N2)
    channel_back(N0, [lambda: reduce_step(late, N0), second, third, lambda: reduce_step(late, N3)])
    xa_copy.wait()
    token_back(N0, [(N5, lambda: advance(layer0, N0))])

    @pl.loop(N0, STRIPS)
    def _(i):
        add_row('b_stem', N0, row_sum(get(grad, strip_rows(i))))
    turn(dout_t, lambda rows: get(grad, rows))
    reduce_send(final, N0)

    def patch_load(k):
        f = (k % N4) * N2 + (other if k < N4 else core)
        images = pl.ds(aligned(coords[N2] * IMAGES, IMAGES), IMAGES)
        return load(patch_hbm.at[:, images, pl.ds(aligned(f * 384, BAND), 384)], pbuf.at[k % N2], k % N2)
    def stem_part(z):
        return g2.at[pl.ds(z * 256, 256), pl.ds(N0, 384)]

    def stem_left():
        for z in range(N2):
            left(stem_part(z), pair_sem.at[N8])
    copies = {N0: patch_load(N0)}
    for k in range(N8):
        if k < N7:
            copies[k + N1] = patch_load(k + N1)
        copies[k].wait()
        y, x = (k % N4) // N2, k % N2
        result = times(dout_t[...], pbuf[k % N2].reshape(ROWS, 384))
        if k < N4:
            if k > N0:
                stem_left()
            g2[:, :384] = result
            for z in range(N2):
                start(stem_part(z), peer[STEM].at[z, y, x], pair_sem.at[N2 * k + z], partner, pair_sem.at[N8])
        else:
            for z in range(N2):
                mine[STEM][z, y, x] = result[z * 256:z * 256 + 256]
        if k == N3:
            stem_left()
            reduce_step(final, N0)
        if k == N5:
            advance(layer0, N1)
    for k in range(N4):
        for z in range(N2):
            arrived(peer[STEM].at[z, k // N2, k % N2], pair_sem.at[N2 * k + z])
    add_peer(STEM)
    phase_send(STEM, N0)
    reduce_step(final, N1)
    advance(layer0, N2, [o1.at[N0], o2.at[N0]])
    reduce_step(final, N2)
    advance([STEM], N0)
    reduce_step(final, N3)
    advance([STEM], N1)
    advance([STEM], N2, [o_stem])
    for copy in pending:
        copy.wait_send()
    for item in range(ITEMS):
        for part in DIMS:
            for phase in DIMS:
                left(phase_source(item, part, phase), send_sem)


def backward_all(*operands):
    any_spec, vmem = pl.BlockSpec(memory_space=pl.ANY), pl.BlockSpec(memory_space=pltpu.VMEM)
    boxes = [pltpu.VMEM((N2,) * (N2 - phase) + (ITEM_SPLITS[item][part][N1], ITEM_SHAPES[item][N1]), F32)
             for item in range(ITEMS) for part in DIMS for phase in DIMS]
    slots = [pltpu.VMEM((N2, N2, N2) + shape, F32) for shape in ITEM_SHAPES]
    plane, blocks = pltpu.VMEM((ROWS, WIDE), F32), pltpu.VMEM((N4, ROWS, BAND), F32)
    plane_bf, turned_bf = pltpu.VMEM((ROWS, WIDE), BF16), pltpu.VMEM((WIDE, ROWS), BF16)
    dma = pltpu.SemaphoreType.DMA
    outs = ((256, 384), (N2, 64, 1024), (N2, 512, 128), (64, 512), (VEC_ROWS, WIDE), (N2, 256, 128))
    return pl.pallas_call(
        backward_kernel, out_shape=[jax.ShapeDtypeStruct(s, F32) for s in outs],
        in_specs=[any_spec] * N2 + [vmem] * N5 + [any_spec] * N2 + [vmem] + [any_spec] * N2 + [vmem], out_specs=[vmem] * len(outs),
        scratch_shapes=slots + slots + boxes + [
            pltpu.VMEM((WIDE, DEEP), BF16), pltpu.VMEM((DEEP, WIDE), BF16), blocks, blocks, blocks, plane,
            plane_bf, turned_bf, plane_bf, turned_bf, plane, plane, plane_bf, plane_bf,
            pltpu.VMEM((N2, N2, N2, 64, WIDE), F32), pltpu.VMEM((WIDE, WIDE), F32),
            pltpu.VMEM((N2, TOK, IMAGES, 384), BF16),
            pltpu.VMEM((256, 256), F32), pltpu.VMEM((256, 128), F32), pltpu.VMEM((N8, WIDE), F32),
            pltpu.VMEM((N4, VEC_ROWS, WIDE), F32), pltpu.VMEM((N2, N4, 256, 128), F32),
            dma, dma((ITEMS, N3, N3)), dma((N2, N3, N4)), dma((9,)), dma((13,)), dma((N3,)), dma((N3, N4))],
        compiler_params=pltpu.CompilerParams(collective_id=N1, has_side_effects=True, vmem_limit_bytes=67043328),
        cost_estimate=pl.CostEstimate(flops=10 ** 9, bytes_accessed=50 * 10 ** N6, transcendentals=N0),
        name='backward')(*operands)


def finish_kernel(*refs):
    take = iter(refs)

    def grab(count):
        return [next(take) for _ in range(count)]
    s_stem, s1, s2, sh, osum, otok = grab(N6)
    loss, o_stem, o1, o2, oh = grab(N5)
    vec_out = grab(len(VECTORS))
    o_b1, o_bt, o_bh, o_t1, o_t2 = grab(N5)
    tp, fsdp = lax.axis_index('tp'), lax.axis_index('fsdp')
    owner = tp * N8 + fsdp
    o_stem[...] = s_stem[...].T
    o1[...] = s1[...]
    oh[...] = sh[:, :CLASSES_HALF]
    block = pltpu.roll(osum[:, pl.ds(aligned(owner // N4 * BAND, BAND), BAND)], BAND - 32 * lax.rem(owner, N4), N1)
    for ref, (name, num) in zip(vec_out, VECTORS):
        at = ROW_VEC[name]
        ref[...] = block[at:at + num, :32]
    deep = osum[:, pl.ds(aligned(lax.rem(owner, N4) * BAND, BAND), BAND)]
    index = lax.broadcasted_iota(jnp.int32, (VEC_ROWS, N1), N0)
    head_row = osum[pl.ds(ROW_VEC['b_head'] + tp, N1), :]
    o_bh[...] = head_row[:, :CLASSES_HALF]
    at = ROW_VEC['loss']
    loss[...] = osum[at:at + N1, :N1]
    for layer in range(N2):
        o2[layer] = s2[layer].T
        chosen = index == ROW_VEC['b_ch1'] + N4 * layer + owner // N4
        o_b1[layer:layer + N1, :] = row_sum(jnp.where(chosen, deep, 0.0))
        found = otok[layer, pl.ds(aligned(fsdp * 32, 32), 32), :]
        o_t1[layer] = found[:, :TOK]
        o_t2[layer] = pltpu.roll(found, 64, N1)[:, :TOK]
        o_bt[layer:layer + N1, :] = found.T[BAND - N8:BAND - N7, :]


def finish_all(*operands):
    vmem = pl.BlockSpec(memory_space=pltpu.VMEM)
    shapes = [(N1, N1), (384, 256), (N2, 64, 1024), (N2, BAND, WIDE), (64, CLASSES_HALF)]
    shapes += [(num, 32) for _, num in VECTORS]
    shapes += [(N2, BAND), (N2, 32), (N1, CLASSES_HALF), (N2, 32, TOK), (N2, 32, TOK)]
    return pl.pallas_call(finish_kernel, out_shape=[jax.ShapeDtypeStruct(shape, F32) for shape in shapes],
                          in_specs=[vmem] * len(operands), out_specs=[vmem] * len(shapes), name='finish')(*operands)


def weight_specs():
    vec_spec = P(CHANNEL_AXES)
    layer_vec = P(None, CHANNEL_AXES)
    return (P('fsdp', 'tp'), vec_spec, layer_vec, layer_vec, P(None, None, 'fsdp'), P(None, 'fsdp'),
            P(None, 'fsdp', None), layer_vec, layer_vec, P(None, 'fsdp', 'tp'), layer_vec,
            P(None, CHANNEL_AXES, None), layer_vec, vec_spec, vec_spec, P('fsdp', 'tp'), P('tp'))


def solution(mesh):
    def step(patches, labels, w_stem, b_stem, ln1_g, ln1_b, w_tok1, b_tok1, w_tok2,
             ln2_g, ln2_b, w_ch1, b_ch1, w_ch2, b_ch2, lnf_g, lnf_b, w_head, b_head):
        def flat(values):
            return values.reshape(N1, -N1)
        by_token = patches.swapaxes(N0, N1)
        w1, w2, xa, xb, t1t, t1, t2, bt, vec, gh, hs, d0 = forward_all(
            by_token, labels.reshape(-N1, N1), w_stem, w_ch1, w_ch2, w_head, flat(b_stem), ln1_g, ln1_b, ln2_g, ln2_b,
            b_ch2, flat(lnf_g), flat(lnf_b), b_ch1, b_tok1, flat(b_head), w_tok1.swapaxes(N1, N2), w_tok2)
        sums = backward_all(w1, w2, t1t, t1, t2, bt, vec, xa, xb, d0, by_token, gh, hs)
        (loss, g_stem, g_ch1, g_ch2, g_head, gb_stem, g1_g, g1_b, g2_g, g2_b, gb_ch2, gf_g, gf_b,
         gb_ch1, gb_tok1, gb_head, g_tok1, g_tok2) = finish_all(*sums)
        return (loss.reshape(()), g_stem, gb_stem.reshape(-N1), g1_g, g1_b, g_tok1.swapaxes(N1, N2), gb_tok1, g_tok2,
                g2_g, g2_b, g_ch1, gb_ch1, g_ch2, gb_ch2, gf_g.reshape(-N1), gf_b.reshape(-N1), g_head,
                gb_head.reshape(-N1))

    specs = weight_specs()
    return jax.shard_map(step, mesh=mesh, in_specs=(P('fsdp', None, None), P('fsdp')) + specs,
                         out_specs=(P(),) + specs, check_vma=False)
```

```python
import functools

import jax
import jax.numpy as jnp
from jax import lax
from jax.experimental import pallas as pl
from jax.experimental.pallas import tpu as pltpu
from jax.sharding import PartitionSpec as P

EPS = 1e-6
CHANNEL_AXES = ('tp', 'fsdp')
LAYER_NAMES = ('ln1_g', 'ln1_b', 'w_tok1', 'b_tok1', 'w_tok2', 'ln2_g', 'ln2_b', 'w_ch1', 'b_ch1', 'w_ch2', 'b_ch2')
N0, N1, N2, N3, N4, N5, N6, N7, N8 = range(9)
MESH = pl.DeviceIdType.MESH
BF16 = jnp.bfloat16
F32 = jnp.float32
ORDERS = ((N0, N1, N2), (N1, N2, N0), (N2, N0, N1))


def my_position():
    tp, fsdp = lax.axis_index('tp'), lax.axis_index('fsdp')
    return (lax.rem(fsdp // N2, N2), fsdp // N4, tp), lax.rem(fsdp, N2)


def aligned(value, size):
    return value if isinstance(value, int) else pl.multiple_of(value, size)


def odd(value):
    return value % N2 if isinstance(value, int) else lax.rem(value, N2)


def shifted(coords, bits):
    return tuple(N1 - c if b else c for c, b in zip(coords, bits))


def owner_of(coords, core):
    x, y, z = coords
    return z, y * N4 + x * N2 + core


def device_of(coords, core):
    tp, fsdp = owner_of(coords, core)
    return {'tp': tp, 'fsdp': fsdp}


def unit(dim):
    return tuple(N1 if d == dim else N0 for d in range(N3))


def plus(a, b):
    return tuple((i + j) % N2 for i, j in zip(a, b))


def barrier_signal(coords, core):
    barrier = pltpu.get_barrier_semaphore()
    for dim in range(N3):
        pl.semaphore_signal(barrier, inc=N1, device_id=device_of(shifted(coords, unit(dim)), core), device_id_type=MESH)
    pl.semaphore_signal(barrier, inc=N1, device_id=device_of(coords, N1 - core), device_id_type=MESH)


def barrier_wait():
    pl.semaphore_wait(pltpu.get_barrier_semaphore(), N4)


ROW_VEC = dict(b_stem=N0, ln1_g=N1, ln1_b=N3, ln2_g=N5, ln2_b=N7, b_ch2=9, b_ch1=11, lnf_g=19, lnf_b=20, b_head=21, loss=23)
VEC_ROWS = 24
TOK = 49
IMAGES = 16
ROWS = TOK * IMAGES
BAND = 128
STRIP = 112
STRIPS = ROWS // STRIP
WIDE = 512
DEEP = 2048
GELU_A = 0.7978845608028654
GELU_B = 0.044715


def by_rows(left, right):
    return lax.dot_general(left, right, (((N1,), (N1,)), ((), ())), preferred_element_type=F32)


def times(left, right):
    return jnp.dot(left, right, preferred_element_type=F32)


def gelu_pair(pre):
    square = pre * pre
    tanh = jnp.tanh(pre * (GELU_A + (GELU_A * GELU_B) * square))
    cdf = 0.5 + 0.5 * tanh
    value = pre * cdf
    return value, cdf + value * ((1.0 - tanh) * (GELU_A + (3.0 * GELU_A * GELU_B) * square))


def gelu_value(pre):
    return pre * (0.5 + 0.5 * jnp.tanh(pre * (GELU_A + (GELU_A * GELU_B) * (pre * pre))))


def image_rows(b):
    return pl.ds(b, TOK, stride=IMAGES)


def get(ref, rows):
    return jnp.concatenate([ref[k, rows, :] for k in range(N4)], axis=N1)


def put(ref, rows, values):
    for k in range(N4):
        ref[k, rows, :] = values[:, k * BAND:(k + N1) * BAND]


def strip_rows(i):
    return pl.ds(aligned(i * STRIP, STRIP), STRIP)


def turn(dst, read):
    whole = ROWS // BAND

    @pl.loop(N0, whole)
    def _(i):
        rows = pl.ds(aligned(i * BAND, BAND), BAND)
        dst[:, rows] = read(rows).astype(F32).T.astype(BF16)
    dst[:, whole * BAND:] = read(pl.ds(whole * BAND, ROWS % BAND)).astype(F32).T.astype(BF16)


def standardize(values):
    centered = values - jnp.mean(values, axis=N1, keepdims=True)
    inv_std = lax.rsqrt(jnp.mean(centered * centered, axis=N1, keepdims=True) + EPS)
    return centered * inv_std, inv_std


def norm_back(grad_out, gain, standard, inv_std):
    grad_std = grad_out * gain
    first = jnp.mean(grad_std, axis=N1, keepdims=True)
    second = jnp.mean(grad_std * standard, axis=N1, keepdims=True)
    return inv_std * (grad_std - first - standard * second)


def row_sum(values):
    return jnp.sum(values, axis=N0, keepdims=True)


DIMS = range(N3)


STEM_W, SMALL, HEAD_W, CHAN1, CHAN2 = N0, N1, N6, (N2, N4), (N3, N5)
GATHER_SPLITS = (((N0, 128), (128, 128), (256, 128)), ((N0, 32), (32, 32), (64, 24)),
                 ((N0, 16), (16, 16), (32, 32)), ((N0, 48), (48, 48), (96, 32)),
                 ((N0, 16), (16, 16), (32, 32)), ((N0, 48), (48, 48), (96, 32)), ((N0, 32), (32, 16), (48, 16)))
GATHERED = len(GATHER_SPLITS)
PACK_ROWS = 88
AT_B1, AT_BT, AT_BH, AT_T = 16, 18, 20, 24
VECTORS = (('b_stem', N1), ('ln1_g', N2), ('ln1_b', N2), ('ln2_g', N2), ('ln2_b', N2), ('b_ch2', N2), ('lnf_g', N1), ('lnf_b', N1))
CLASSES_HALF = 500
TOTAL = 256
PATCH = 3072


def forward_kernel(*refs):
    take = iter(refs)

    def grab(count):
        return [next(take) for _ in range(count)]
    patch_hbm, labels, f_stem, f1, f2, f_head = grab(N6)
    vec_in = grab(len(VECTORS))
    i_b1, i_bt, i_bh, i_t1, i_t2 = grab(N5)
    w1_out, w2_out, xa_out, xb_out, t1t, t1, t2, bt, vec, gh, hs, d0 = grab(12)
    own_stem, own1, own2, own_head, pack = grab(N5)
    stem_w, small, w1, w2, head_w = grab(N5)
    pin, t2t = grab(N2)
    xs = grab(N5)
    v, pre, act, pooled = grab(N4)
    send_sem, recv_sem, load_sem, save_sem = grab(N4)
    coords, core = my_position()
    tp = coords[N2]
    barrier_signal(coords, core)
    patch_copy = pltpu.make_async_copy(patch_hbm.at[:, pl.ds(aligned(tp * IMAGES, IMAGES), IMAGES), :], pin, load_sem)
    patch_copy.start()

    own_stem[...] = f_stem[...].astype(BF16)
    own1[...] = f1[...].astype(BF16)
    own2[...] = f2[...].astype(BF16)
    own_head[...] = jnp.zeros(own_head.shape, BF16)
    own_head[:, :CLASSES_HALF] = f_head[...].astype(BF16)
    pack[...] = jnp.zeros(pack.shape, F32)
    row = N0
    for ref, (_, num) in zip(vec_in, VECTORS):
        pack[row:row + num, :32] = ref[...]
        row += num
    pack[AT_B1:AT_B1 + N2, :] = i_b1[...]
    pack[AT_BT:AT_BT + N2, :32] = i_bt[...]
    for k in range(N4):
        width = min(BAND, CLASSES_HALF - k * BAND)
        pack[AT_BH + k:AT_BH + k + N1, :width] = i_bh[:, k * BAND:k * BAND + width]
    for layer in range(N2):
        at = AT_T + 32 * layer
        pack[at:at + 32, :TOK] = i_t1[layer]
        pack[at:at + 32, 64:64 + TOK] = i_t2[layer]
    barrier_wait()

    own = [own_stem, pack, own1.at[N0], own2.at[N0], own1.at[N1], own2.at[N1], own_head]

    def block(item, tp, fsdp, lo, num):
        if item == STEM_W:
            return stem_w.at[pl.ds(aligned(fsdp * 384 + lo, 128), num), pl.ds(aligned(tp * 256, 128), 256)]
        if item == SMALL:
            return small.at[tp * N8 + fsdp, pl.ds(lo, num), :]
        if item in CHAN1:
            return w1.at[CHAN1.index(item), pl.ds(aligned(fsdp * 64 + lo, 16), num), pl.ds(aligned(tp * 1024, 128), 1024)]
        if item in CHAN2:
            return w2.at[CHAN2.index(item), pl.ds(aligned((tp * N8 + fsdp) * 128 + lo, 16), num), :]
        return head_w.at[pl.ds(aligned(fsdp * 64 + lo, 16), num), pl.ds(aligned(tp * WIDE, 128), WIDE)]

    def blocks(item, num):
        rows, cols = own[item].shape
        if item == SMALL:
            return small.at[pl.ds(N0, num)]
        if item in CHAN1:
            return w1.at[CHAN1.index(item), pl.ds(N0, num * rows), pl.ds(N0, cols)]
        if item in CHAN2:
            return w2.at[CHAN2.index(item), pl.ds(N0, num * rows), pl.ds(N0, cols)]
        return (stem_w if item == STEM_W else head_w).at[pl.ds(N0, num * rows), pl.ds(N0, cols)]

    def arrivals(item, num, slot):
        view = blocks(item, num)
        pltpu.make_async_remote_copy(src_ref=view, dst_ref=view, send_sem=send_sem.at[item],
                                     recv_sem=recv_sem.at[item, slot], device_id=device_of(coords, core),
                                     device_id_type=MESH).wait_recv()

    def move(item, part, bits, is_own, target, slot):
        lo, num = GATHER_SPLITS[item][part]
        there = block(item, *owner_of(shifted(coords, bits), core), lo, num)
        here = own[item].at[pl.ds(lo, num), :] if is_own else there
        pltpu.make_async_remote_copy(src_ref=here, dst_ref=there, send_sem=send_sem.at[item],
                                     recv_sem=recv_sem.at[item, slot], device_id=target,
                                     device_id_type=MESH).start()

    def pass_on(item, part, bits, level):
        for step in range(level, N3):
            move(item, part, bits, False, device_of(shifted(coords, unit(ORDERS[part][step])), core), step)
        move(item, part, bits, False, device_of(coords, N1 - core), N3)

    def bits_of(part, rank):
        bits = [N0, N0, N0]
        for i in DIMS:
            bits[ORDERS[part][i]] = (rank >> i) % N2
        return tuple(bits)

    def send_own(item):
        none = (N0, N0, N0)
        for step in DIMS:
            for part in DIMS:
                target = device_of(shifted(coords, unit(ORDERS[part][step])), core)
                move(item, part, none, True, target, step)
        for part in DIMS:
            move(item, part, none, True, device_of(coords, N1 - core), N3)

    def forward(item, level):
        arrivals(item, N2 ** level, level)
        for rank in range(N2 ** level):
            for part in DIMS:
                pass_on(item, part, bits_of(part, rank + N2 ** level), level + N1)

    def finish(item):
        arrivals(item, N8, N3)

    def place_own(item):
        here = own[item]
        block(item, *owner_of(coords, core), N0, here.shape[N0])[...] = here[...]

    saves = []

    def save(src, dst):
        copy = pltpu.make_async_copy(src, dst, save_sem.at[len(saves)])
        copy.start()
        saves.append((src, dst))

    early = (SMALL, STEM_W)
    for item in early:
        send_own(item)
    for item in range(GATHERED):
        place_own(item)
    for level in range(N2):
        for item in early:
            forward(item, level)
    send_own(CHAN1[N0])
    for item in early:
        forward(item, N2)
    send_own(CHAN2[N0])
    finish(SMALL)

    lane32 = lax.broadcasted_iota(jnp.int32, (N1, BAND), N1) // 32

    def lay_out(q, lo, num):
        total = None
        for i in range(N4):
            piece = small[N4 * q + i, lo:lo + num, :]
            piece = jnp.where(lane32 == i, pltpu.roll(piece, 32 * i, N1) if i else piece, 0.0)
            total = piece if total is None else total + piece
        return total
    vec[...] = jnp.zeros(vec.shape, F32)
    rows_first, lnf = ROW_VEC['b_ch1'], ROW_VEC['lnf_g']
    for q in range(N4):
        cols = slice(q * BAND, q * BAND + BAND)
        found = lay_out(q, N0, 16)
        vec[:rows_first, cols] = found[:rows_first]
        vec[lnf:lnf + N2, cols] = found[rows_first:rows_first + N2]
        for layer in range(N2):
            for j in range(N4):
                at = rows_first + N4 * layer + j
                vec[at:at + N1, cols] = small[N4 * j + q, AT_B1 + layer:AT_B1 + layer + N1, :]
        for z in range(N2):
            at = ROW_VEC['b_head'] + z
            vec[at:at + N1, cols] = small[N8 * z, AT_BH + q:AT_BH + q + N1, :]
    for q in range(N2):
        cols = slice(q * BAND, q * BAND + BAND)
        turned = lay_out(q, AT_B1, N8).T
        for layer in range(N2):
            column = AT_BT - AT_B1 + layer
            bt[layer, cols, :] = turned[:, column:column + N1]
            at = AT_T + 32 * layer
            rows = jnp.concatenate([small[N4 * q + i, at:at + 32, :] for i in range(N4)], axis=N0)
            back = rows.T
            t1t[layer, cols, :] = rows[:, :TOK].astype(BF16)
            t1[layer, :, cols] = back[:TOK].astype(BF16)
            t2[layer, cols, :] = pltpu.roll(rows, 64, N1)[:, :TOK].astype(BF16)
            t2t[layer, :, cols] = back[64:64 + TOK].astype(BF16)

    def vector(name, at=N0):
        return vec[pl.ds(ROW_VEC[name] + at, N1), :]

    forward(CHAN1[N0], N0)
    finish(STEM_W)
    patch_copy.wait()
    cut = TOK // N2 + N1
    for lo, num, tasks in ((N0, cut, ((CHAN2[N0], N0), (CHAN1[N0], N1))), (cut, TOK - cut, ((CHAN2[N0], N1),))):
        rows = pl.ds(lo * IMAGES, num * IMAGES)
        patches = pin[lo:lo + num].reshape(num * IMAGES, PATCH)
        put(xs[N0], rows, times(patches, stem_w[...]) + vector('b_stem'))
        for item, level in tasks:
            forward(item, level)
        send_own(CHAN2[N1] if lo else CHAN1[N1])
    save(xs[N0], xa_out.at[N0])

    def token_mix(layer, tasks):
        source, target = xs[N2 * layer], xs[N2 * layer + N1]
        gain, shift = vector('ln1_g', layer), vector('ln1_b', layer)

        @pl.loop(N0, IMAGES // N2)
        def _(pair):
            rows = [image_rows(N2 * pair + i) for i in range(N2)]
            here = [get(source, r) for r in rows]
            norm = [(standardize(x)[N0] * gain + shift).astype(BF16) for x in here]
            hidden = [gelu_value(times(t1t[layer], n) + bt[layer]).astype(BF16) for n in norm]
            mixed = [x + times(t2t[layer], h) for x, h in zip(here, hidden)]
            for r, x in zip(rows, mixed):
                put(target, r, x)
            for k, task in enumerate(tasks):
                pl.when(pair == k)(task)

    def channel_mix(layer, tasks):
        source, target = xs[N2 * layer + N1], xs[N2 * layer + N2]
        gain, shift = vector('ln2_g', layer), vector('ln2_b', layer)

        @pl.loop(N0, STRIPS)
        def _(i):
            rows = strip_rows(i)
            here = get(source, rows)
            v[rows, :] = (standardize(here)[N0] * gain + shift).astype(BF16)
            put(target, rows, here + vector('b_ch2', layer))

        @pl.loop(N0, N4)
        def _(j):
            cols = pl.ds(aligned(j * WIDE, WIDE), WIDE)
            bias = vector('b_ch1', N4 * layer + j)
            pre[...] = times(v[...], w1[layer, :, cols])

            @pl.loop(N0, STRIPS)
            def _(i):
                rows = strip_rows(i)
                act[rows, :] = gelu_value(pre[rows, :] + bias).astype(BF16)
            everything = pl.ds(N0, ROWS)
            put(target, everything, get(target, everything) + times(act[...], w2[layer, cols, :]))
            for k, task in enumerate(tasks):
                pl.when(j == k)(task)

    def both(first, second):
        def run():
            first()
            second()
        return run

    def step(item, level):
        return lambda: forward(item, level)
    token_mix(N0, [step(CHAN1[N0], N2), step(CHAN2[N0], N2), both(step(CHAN1[N1], N0), lambda: send_own(HEAD_W)),
                  step(CHAN2[N1], N0), step(CHAN1[N1], N1), step(CHAN2[N1], N1), step(HEAD_W, N0), step(CHAN1[N1], N2)])
    save(xs[N1], xb_out.at[N0])
    finish(CHAN1[N0])
    finish(CHAN2[N0])
    save(w1.at[N0], w1_out.at[N0])
    save(w2.at[N0], w2_out.at[N0])
    channel_mix(N0, [step(CHAN2[N1], N2), step(HEAD_W, N1), step(HEAD_W, N2)])
    save(xs[N2], xa_out.at[N1])
    token_mix(N1, [])
    save(xs[N3], xb_out.at[N1])
    for item in (CHAN1[N1], CHAN2[N1], HEAD_W):
        finish(item)
    save(w1.at[N1], w1_out.at[N1])
    save(w2.at[N1], w2_out.at[N1])
    channel_mix(N1, [])

    pooled[...] = jnp.zeros(pooled.shape, F32)

    @pl.loop(N0, TOK)
    def _(t):
        pooled[...] = pooled[...] + get(xs[N4], pl.ds(aligned(t * IMAGES, IMAGES), IMAGES))
    gain = vector('lnf_g')
    standard, inv_std = standardize(pooled[...] * (1.0 / TOK))
    norm = standard * gain + vector('lnf_b')
    norm_bf = norm.astype(BF16)
    lane = lax.broadcasted_iota(jnp.int32, (IMAGES, WIDE), N1)
    real = lane < CLASSES_HALF
    logits = [times(norm_bf, head_w[:, z * WIDE:z * WIDE + WIDE]) + vector('b_head', z) for z in range(N2)]
    row_max = jnp.maximum(*[jnp.max(jnp.where(real, l, -jnp.inf), axis=N1, keepdims=True) for l in logits])
    exps = [jnp.where(real, jnp.exp(jnp.where(real, l, row_max) - row_max), 0.0) for l in logits]
    sums = jnp.sum(exps[N0], axis=N1, keepdims=True) + jnp.sum(exps[N1], axis=N1, keepdims=True)
    square = (IMAGES, labels.shape[N1])
    chosen = lax.broadcasted_iota(jnp.int32, square, N1) == lax.broadcasted_iota(jnp.int32, square, N0) + tp * IMAGES
    mine = jnp.sum(jnp.where(chosen, labels[...].astype(F32), 0.0), axis=N1, keepdims=True).astype(jnp.int32)
    hits = [jnp.logical_and(lane + z * CLASSES_HALF == mine, real) for z in range(N2)]
    picked = sum(jnp.sum(jnp.where(hit, l, 0.0), axis=N1, keepdims=True) for hit, l in zip(hits, logits))
    losses = row_max + jnp.log(sums) - picked
    hs[...] = jnp.zeros(hs.shape, F32)
    turned = norm.T.astype(BF16)
    back = None
    for z in range(N2):
        d_logits = (exps[z] / sums - hits[z].astype(F32)) * (1.0 / TOTAL)
        d_logits_bf = d_logits.astype(BF16)
        gh[:, z * WIDE:z * WIDE + WIDE] = times(turned, d_logits_bf)
        at = ROW_VEC['b_head'] + z
        hs[at:at + N1, :] = row_sum(d_logits)
        piece = by_rows(d_logits_bf, head_w[:, z * WIDE:z * WIDE + WIDE])
        back = piece if back is None else back + piece
    hs[lnf:lnf + N1, :] = row_sum(back * standard)
    hs[lnf + N1:lnf + N2, :] = row_sum(back)
    at = ROW_VEC['loss']
    hs[at:at + N1, :] = jnp.broadcast_to(row_sum(losses) * (1.0 / TOTAL), (N1, WIDE))
    d0[...] = norm_back(back, gain, standard, inv_std) * (1.0 / TOK)

    for k, (src, dst) in enumerate(saves):
        pltpu.make_async_copy(src, dst, save_sem.at[k]).wait()
    whole = [stem_w, small, w1.at[N0], w2.at[N0], w1.at[N1], w2.at[N1], head_w]
    for item, ref in enumerate(whole):
        view = ref.at[pl.ds(N0, ref.shape[N0] // 16 * 15)]
        pltpu.make_async_remote_copy(src_ref=view, dst_ref=view, send_sem=send_sem.at[item],
                                     recv_sem=recv_sem.at[item, N0], device_id=device_of(coords, core),
                                     device_id_type=MESH).wait_send()


def forward_all(*operands):
    any_spec, vmem = pl.BlockSpec(memory_space=pl.ANY), pl.BlockSpec(memory_space=pltpu.VMEM)
    shape = jax.ShapeDtypeStruct
    plane, blocks = (ROWS, WIDE), (N4, ROWS, BAND)
    outs = [shape((N2, WIDE, DEEP), BF16), shape((N2, DEEP, WIDE), BF16), shape((N2,) + blocks, F32),
            shape((N2,) + blocks, F32), shape((N2, 256, TOK), BF16),
            shape((N2, TOK, 256), BF16), shape((N2, 256, TOK), BF16), shape((N2, 256, N1), F32),
            shape((VEC_ROWS, WIDE), F32), shape((WIDE, N2 * WIDE), F32), shape((VEC_ROWS, WIDE), F32),
            shape((IMAGES, WIDE), F32)]
    dma = pltpu.SemaphoreType.DMA
    return pl.pallas_call(
        forward_kernel, out_shape=outs, in_specs=[any_spec] + [vmem] * (len(operands) - N1),
        out_specs=[any_spec] * N4 + [vmem] * N8,
        scratch_shapes=[
            pltpu.VMEM((384, 256), BF16), pltpu.VMEM((N2, 64, 1024), BF16), pltpu.VMEM((N2, 128, WIDE), BF16),
            pltpu.VMEM((64, WIDE), BF16), pltpu.VMEM((PACK_ROWS, BAND), F32),
            pltpu.VMEM((PATCH, WIDE), BF16), pltpu.VMEM((16, PACK_ROWS, BAND), F32), pltpu.VMEM((N2, WIDE, DEEP), BF16),
            pltpu.VMEM((N2, DEEP, WIDE), BF16), pltpu.VMEM((WIDE, N2 * WIDE), BF16),
            pltpu.VMEM((TOK, IMAGES, PATCH), BF16),
            pltpu.VMEM((N2, TOK, 256), BF16)] + [pltpu.VMEM(blocks, F32)] * N5 + [
            pltpu.VMEM(plane, BF16), pltpu.VMEM(plane, F32), pltpu.VMEM(plane, BF16),
            pltpu.VMEM((IMAGES, WIDE), F32),
            dma((GATHERED,)), dma((GATHERED, N4)), dma, dma((N8,))],
        compiler_params=pltpu.CompilerParams(collective_id=N0, has_side_effects=True, vmem_limit_bytes=67043328),
        cost_estimate=pl.CostEstimate(flops=10 ** 9, bytes_accessed=25 * 10 ** N6, transcendentals=N0),
        name='forward')(*operands)


HEAD, CH1, CH2, STEM = N0, (N1, N3), (N2, N4), N5
ITEM_SHAPES = ((64, 512), (64, 1024), (512, 128), (64, 1024), (512, 128), (256, 384))
ITEM_SPLITS = tuple(tuple((lo, hi - lo) for lo, hi in zip((N0,) + cut, cut + (shape[N0],)))
                    for shape, cut in zip(ITEM_SHAPES, ((24, 48), (24, 48), (176, 344), (24, 48), (176, 344), (88, 176))))
ITEMS = len(ITEM_SHAPES)


def backward_kernel(*refs):
    take = iter(refs)

    def grab(count):
        return [next(take) for _ in range(count)]
    w1_hbm, w2_hbm, t1t, t1, t2, bt, vec, xa_hbm, xb_hbm, d0, patch_hbm, gh_hbm, hs = grab(13)
    o_stem, o1, o2, oh, osum, otok = grab(N6)
    mine, peer = grab(ITEMS), grab(ITEMS)
    boxes = [[grab(N3) for _ in DIMS] for _ in range(ITEMS)]
    w1, w2, xa, xb, grad, acc, v, vt, dout, dout_t, pre, dact, act, dpre, g1, g2, pbuf = grab(17)
    tacc1, tacc2, bacc, sbox, tbox = grab(N5)
    send_sem, hop_sem, peer_sem, pair_sem, load_sem, red_send, red_recv = grab(N7)
    coords, core = my_position()
    other = N1 - core
    barrier_signal(coords, core)
    partner = device_of(coords, other)
    pending = []

    def start(src, dst, sem, device, sent=None):
        copy = pltpu.make_async_remote_copy(src_ref=src, dst_ref=dst, send_sem=send_sem if sent is None else sent,
                                            recv_sem=sem, device_id=device, device_id_type=MESH)
        copy.start()
        return copy

    def arrived(dst, sem):
        pltpu.make_async_remote_copy(src_ref=dst, dst_ref=dst, send_sem=send_sem, recv_sem=sem,
                                     device_id=partner, device_id_type=MESH).wait_recv()

    def left(src, sent):
        pltpu.make_async_remote_copy(src_ref=src, dst_ref=src, send_sem=sent, recv_sem=pair_sem.at[N0],
                                     device_id=partner, device_id_type=MESH).wait_send()

    def view(ref, item, part, select):
        lo, num = ITEM_SPLITS[item][part]
        x, y, z = select
        return ref.at[z, y, x, pl.ds(lo, num), :]

    def phase_source(item, part, phase):
        order = ORDERS[part]
        select = [pl.ds(N0, N2)] * N3
        for dim in order[:phase]:
            select[dim] = coords[dim]
        select[order[phase]] = N1 - coords[order[phase]]
        return view(mine[item], item, part, select)

    def phase_send(item, phase):
        for part in DIMS:
            start(phase_source(item, part, phase), boxes[item][part][phase], hop_sem.at[item, part, phase],
                  device_of(shifted(coords, unit(ORDERS[part][phase])), core))

    def phase_take(item, phase, final=None):
        for part in DIMS:
            order = ORDERS[part]
            box = boxes[item][part][phase]
            arrived(box, hop_sem.at[item, part, phase])
            rest = [dim for dim in (N2, N1, N0) if dim in order[phase + N1:]]
            for sub in range(N2 ** len(rest)):
                bits = [(sub >> place) % N2 for place in range(len(rest))]
                select = list(coords)
                for dim, bit in zip(rest, bits):
                    select[dim] = bit
                here = view(mine[item], item, part, select)
                total = here[...] + (box.at[tuple(bits)] if bits else box)[...]
                if final is None:
                    here[...] = total
                else:
                    lo, num = ITEM_SPLITS[item][part]
                    final[pl.ds(lo, num), :] = total

    def add_peer(item):
        @pl.loop(N0, N8)
        def _(i):
            at = (i // N4, odd(i // N2), odd(i))
            mine[item][at] = mine[item][at] + peer[item][at]

    def advance(items, phase, finals=None):
        for index, item in enumerate(items):
            phase_take(item, phase, None if finals is None else finals[index])
            if phase < N2:
                phase_send(item, phase + N1)

    def reduce_send(parts, stage):
        device = partner if stage == N0 else device_of(shifted(coords, unit(stage - N1)), core)
        for ref, box, slot in parts:
            start(ref, box.at[stage], red_recv.at[slot, stage], device, red_send.at[slot])

    def reduce_take(parts, stage):
        for ref, box, slot in parts:
            arrived(box.at[stage], red_recv.at[slot, stage])
            left(ref, red_send.at[slot])
            ref[...] = ref[...] + box[stage]

    def reduce_step(parts, stage):
        reduce_take(parts, stage)
        if stage < N3:
            reduce_send(parts, stage + N1)

    def load(src, dst, slot):
        copy = pltpu.make_async_copy(src, dst, load_sem.at[slot])
        copy.start()
        return copy

    def head_view(f):
        return gh_hbm.at[pl.ds(aligned(f * 64, 64), 64), :]
    first = [load(w1_hbm.at[N1], w1, N0), load(w2_hbm.at[N1], w2, N1), load(xb_hbm.at[N1], xb, N2)]
    xa_copy = load(xa_hbm.at[N1], xa, N4)
    osum[...] = hs[...]

    @pl.loop(N0, TOK)
    def _(t):
        put(grad, pl.ds(aligned(t * IMAGES, IMAGES), IMAGES), d0[...])
    barrier_wait()
    heads = []
    for y in range(N2):
        for x in range(N2):
            for z in range(N2):
                slot = y * N4 + x * N2 + z
                pending.append(start(head_view(y * N4 + x * N2 + other).at[:, pl.ds(z * WIDE, WIDE)],
                                     peer[HEAD].at[z, y, x], pair_sem.at[slot], partner))
                heads.append(load(head_view(y * N4 + x * N2 + core).at[:, pl.ds(z * WIDE, WIDE)],
                                  mine[HEAD].at[z, y, x], N5 + slot))

    def head_start():
        for y in range(N2):
            for x in range(N2):
                for z in range(N2):
                    slot = y * N4 + x * N2 + z
                    heads[slot].wait()
                    arrived(peer[HEAD].at[z, y, x], pair_sem.at[slot])
        add_peer(HEAD)
        phase_send(HEAD, N0)

    def add_row(name, at, values):
        row = pl.ds(ROW_VEC[name] + at, N1)
        osum[row, :] = osum[row, :] + values

    def chunk_moves(layer, j):
        z, y = j // N2, odd(j)
        moves = [(g1.at[:, :, other], peer[CH1[layer]].at[z, :, :, :, pl.ds(aligned(y * WIDE, WIDE), WIDE)])]
        for x in range(N2):
            moves.append((g2.at[:, pl.ds(aligned((N2 * x + other) * BAND, BAND), BAND)],
                          peer[CH2[layer]].at[z, y, x]))
        return [(src, dst, peer_sem.at[layer, k, j]) for k, (src, dst) in enumerate(moves)]

    def channel_back(layer, steps):
        gain, shift = vec[pl.ds(ROW_VEC['ln2_g'] + layer, N1), :], vec[pl.ds(ROW_VEC['ln2_b'] + layer, N1), :]

        @pl.loop(N0, STRIPS)
        def _(i):
            rows = strip_rows(i)
            standard, _ = standardize(get(xb, rows))
            v[rows, :] = (standard * gain + shift).astype(BF16)
            here = get(grad, rows)
            dout[rows, :] = here.astype(BF16)
            add_row('b_ch2', layer, row_sum(here))
            acc[rows, :] = jnp.zeros((STRIP, WIDE), F32)
        turn(vt, lambda rows: v[rows, :])
        turn(dout_t, lambda rows: dout[rows, :])

        @pl.loop(N0, N4)
        def _(j):
            cols = pl.ds(aligned(j * WIDE, WIDE), WIDE)
            bias = vec[pl.ds(ROW_VEC['b_ch1'] + N4 * layer + j, N1), :]
            bacc[...] = jnp.zeros(bacc.shape, F32)
            pre[...] = times(v[...], w1[:, cols])
            dact[...] = by_rows(dout[...], w2[cols, :])

            @pl.loop(N0, STRIPS)
            def _(i):
                rows = strip_rows(i)
                value, slope = gelu_pair(pre[rows, :] + bias)
                change = dact[rows, :] * slope
                act[rows, :] = value.astype(BF16)
                dpre[rows, :] = change.astype(BF16)
                bacc[...] = bacc[...] + jnp.sum(change.reshape(STRIP // N8, N8, WIDE), axis=N0)
            acc[...] = acc[...] + by_rows(dpre[...], w1[:, cols])
            add_row('b_ch1', N4 * layer + j, row_sum(bacc[...]))

            @pl.when(j > N0)
            def _():
                for src, _, _ in chunk_moves(layer, j):
                    left(src, pair_sem.at[N8])
            g1[...] = times(vt[...], dpre[...]).reshape(g1.shape)
            g2[...] = times(dout_t[...], act[...])
            for src, dst, sem in chunk_moves(layer, j):
                start(src, dst, sem, partner, pair_sem.at[N8])
            z, y = j // N2, odd(j)
            mine[CH1[layer]][z, :, :, :, pl.ds(aligned(y * WIDE, WIDE), WIDE)] = g1[:, :, core]
            for x in range(N2):
                mine[CH2[layer]][z, y, x] = g2[:, pl.ds(aligned((N2 * x + core) * BAND, BAND), BAND)]
            for k, step in enumerate(steps):
                pl.when(j == k)(step)
        for src, _, _ in chunk_moves(layer, N3):
            left(src, pair_sem.at[N8])
        for j in range(N4):
            for _, dst, sem in chunk_moves(layer, j):
                arrived(dst, sem)
        for item in (CH1[layer], CH2[layer]):
            add_peer(item)
            phase_send(item, N0)

        @pl.loop(N0, STRIPS)
        def _(i):
            rows = strip_rows(i)
            standard, inv_std = standardize(get(xb, rows))
            here = acc[rows, :]
            add_row('ln2_g', layer, row_sum(here * standard))
            add_row('ln2_b', layer, row_sum(here))
            put(grad, rows, get(grad, rows) + norm_back(here, gain, standard, inv_std))

    def token_back(layer, steps):
        gain, shift = vec[pl.ds(ROW_VEC['ln1_g'] + layer, N1), :], vec[pl.ds(ROW_VEC['ln1_b'] + layer, N1), :]
        tacc1[...] = jnp.zeros(tacc1.shape, F32)
        tacc2[...] = jnp.zeros(tacc2.shape, F32)

        @pl.loop(N0, IMAGES // N2)
        def _(pair):
            rows = [image_rows(N2 * pair + i) for i in range(N2)]
            both = range(len(rows))
            inputs, heres = [get(xa, r) for r in rows], [get(grad, r) for r in rows]
            standards, invs = zip(*[standardize(x) for x in inputs])
            norms = [(x * gain + shift).astype(BF16) for x in standards]
            heres_bf = [x.astype(BF16) for x in heres]
            values, slopes = zip(*[gelu_pair(times(t1t[layer], x) + bt[layer]) for x in norms])
            changes = [times(t2[layer], x) * slope for x, slope in zip(heres_bf, slopes)]
            changes_bf = [x.astype(BF16) for x in changes]
            total = sum(x[:, k * BAND:(k + N1) * BAND] for x in changes for k in range(N4))
            d_norms = [times(t1[layer], x) for x in changes_bf]
            tacc1[:, BAND:] = tacc1[:, BAND:] + total
            tacc1[:, :TOK] = tacc1[:, :TOK] + sum(by_rows(changes_bf[i], norms[i]) for i in both)
            tacc2[:, :TOK] = tacc2[:, :TOK] + sum(by_rows(values[i].astype(BF16), heres_bf[i]) for i in both)
            add_row('ln1_g', layer, sum(row_sum(d_norms[i] * standards[i]) for i in both))
            add_row('ln1_b', layer, sum(row_sum(d_norms[i]) for i in both))
            results = [heres[i] + norm_back(d_norms[i], gain, standards[i], invs[i]) for i in both]
            for r, x in zip(rows, results):
                put(grad, r, x)
            for k, step in steps:
                pl.when(pair == k)(step)
        lane = lax.broadcasted_iota(jnp.int32, (256, BAND), N1)
        bias_grad = jnp.sum(tacc1[:, BAND:], axis=N1, keepdims=True)
        otok[layer] = (jnp.where(lane < TOK, tacc1[:, :BAND], 0.0)
                       + pltpu.roll(jnp.where(lane < TOK, tacc2[...], 0.0), 64, N1)
                       + jnp.where(lane == BAND - N8, bias_grad, 0.0))

    late = [(otok.at[N1], tbox.at[N1], N1)]
    final = [(otok.at[N0], tbox.at[N0], N0), (osum, sbox, N2)]
    layer1, layer0 = (CH1[N1], CH2[N1]), (CH1[N0], CH2[N0])

    def nothing():
        pass

    for copy in first:
        copy.wait()
    channel_back(N1, [head_start, nothing, lambda: advance([HEAD], N0), lambda: advance([HEAD], N1)])
    again = [load(w1_hbm.at[N0], w1, N0), load(w2_hbm.at[N0], w2, N1), load(xb_hbm.at[N0], xb, N2)]
    xa_copy.wait()
    token_back(N1, [(N1, lambda: advance([HEAD], N2, [oh])), (N7, lambda: advance(layer1, N0))])
    reduce_send(late, N0)
    xa_copy = load(xa_hbm.at[N0], xa, N4)
    for copy in again:
        copy.wait()

    def last():
        advance(layer1, N1)
        reduce_step(late, N1)
    channel_back(N0, [nothing, lambda: reduce_step(late, N0), nothing, last])
    xa_copy.wait()
    token_back(N0, [(N2, lambda: advance(layer1, N2, [o1.at[N1], o2.at[N1]])), (N3, lambda: reduce_step(late, N2)),
                   (N7, lambda: advance(layer0, N0))])

    @pl.loop(N0, STRIPS)
    def _(i):
        add_row('b_stem', N0, row_sum(get(grad, strip_rows(i))))
    turn(dout_t, lambda rows: get(grad, rows))
    reduce_send(final, N0)

    def patch_load(k):
        f = (k % N4) * N2 + (other if k < N4 else core)
        images = pl.ds(aligned(coords[N2] * IMAGES, IMAGES), IMAGES)
        return load(patch_hbm.at[:, images, pl.ds(aligned(f * 384, BAND), 384)], pbuf.at[k % N2], k % N2)
    def stem_part(z):
        return g2.at[pl.ds(z * 256, 256), pl.ds(N0, 384)]

    def stem_left():
        for z in range(N2):
            left(stem_part(z), pair_sem.at[N8])
    copies = {N0: patch_load(N0)}
    for k in range(N8):
        if k < N7:
            copies[k + N1] = patch_load(k + N1)
        copies[k].wait()
        y, x = (k % N4) // N2, k % N2
        result = times(dout_t[...], pbuf[k % N2].reshape(ROWS, 384))
        if k < N4:
            if k > N0:
                stem_left()
            g2[:, :384] = result
            for z in range(N2):
                start(stem_part(z), peer[STEM].at[z, y, x], pair_sem.at[N2 * k + z], partner, pair_sem.at[N8])
        else:
            for z in range(N2):
                mine[STEM][z, y, x] = result[z * 256:z * 256 + 256]
        if k == N3:
            stem_left()
            reduce_step(final, N0)
    for k in range(N4):
        for z in range(N2):
            arrived(peer[STEM].at[z, k // N2, k % N2], pair_sem.at[N2 * k + z])
    add_peer(STEM)
    phase_send(STEM, N0)
    reduce_step(late, N3)
    reduce_step(final, N1)
    advance(layer0, N1)
    advance([STEM], N0)
    reduce_step(final, N2)
    advance(layer0, N2, [o1.at[N0], o2.at[N0]])
    advance([STEM], N1)
    reduce_step(final, N3)
    advance([STEM], N2, [o_stem])
    for copy in pending:
        copy.wait_send()
    for item in range(ITEMS):
        for part in DIMS:
            for phase in DIMS:
                left(phase_source(item, part, phase), send_sem)


def backward_all(*operands):
    any_spec, vmem = pl.BlockSpec(memory_space=pl.ANY), pl.BlockSpec(memory_space=pltpu.VMEM)
    boxes = [pltpu.VMEM((N2,) * (N2 - phase) + (ITEM_SPLITS[item][part][N1], ITEM_SHAPES[item][N1]), F32)
             for item in range(ITEMS) for part in DIMS for phase in DIMS]
    slots = [pltpu.VMEM((N2, N2, N2) + shape, F32) for shape in ITEM_SHAPES]
    plane, blocks = pltpu.VMEM((ROWS, WIDE), F32), pltpu.VMEM((N4, ROWS, BAND), F32)
    plane_bf, turned_bf = pltpu.VMEM((ROWS, WIDE), BF16), pltpu.VMEM((WIDE, ROWS), BF16)
    dma = pltpu.SemaphoreType.DMA
    outs = ((256, 384), (N2, 64, 1024), (N2, 512, 128), (64, 512), (VEC_ROWS, WIDE), (N2, 256, 128))
    return pl.pallas_call(
        backward_kernel, out_shape=[jax.ShapeDtypeStruct(s, F32) for s in outs],
        in_specs=[any_spec] * N2 + [vmem] * N5 + [any_spec] * N2 + [vmem] + [any_spec] * N2 + [vmem], out_specs=[vmem] * len(outs),
        scratch_shapes=slots + slots + boxes + [
            pltpu.VMEM((WIDE, DEEP), BF16), pltpu.VMEM((DEEP, WIDE), BF16), blocks, blocks, blocks, plane,
            plane_bf, turned_bf, plane_bf, turned_bf, plane, plane, plane_bf, plane_bf,
            pltpu.VMEM((N2, N2, N2, 64, WIDE), F32), pltpu.VMEM((WIDE, WIDE), F32),
            pltpu.VMEM((N2, TOK, IMAGES, 384), BF16),
            pltpu.VMEM((256, 256), F32), pltpu.VMEM((256, 128), F32), pltpu.VMEM((N8, WIDE), F32),
            pltpu.VMEM((N4, VEC_ROWS, WIDE), F32), pltpu.VMEM((N2, N4, 256, 128), F32),
            dma, dma((ITEMS, N3, N3)), dma((N2, N3, N4)), dma((9,)), dma((13,)), dma((N3,)), dma((N3, N4))],
        compiler_params=pltpu.CompilerParams(collective_id=N1, has_side_effects=True, vmem_limit_bytes=67043328),
        cost_estimate=pl.CostEstimate(flops=10 ** 9, bytes_accessed=50 * 10 ** N6, transcendentals=N0),
        name='backward')(*operands)


def finish_kernel(*refs):
    take = iter(refs)

    def grab(count):
        return [next(take) for _ in range(count)]
    s_stem, s1, s2, sh, osum, otok = grab(N6)
    loss, o_stem, o1, o2, oh = grab(N5)
    vec_out = grab(len(VECTORS))
    o_b1, o_bt, o_bh, o_t1, o_t2 = grab(N5)
    tp, fsdp = lax.axis_index('tp'), lax.axis_index('fsdp')
    owner = tp * N8 + fsdp
    o_stem[...] = s_stem[...].T
    o1[...] = s1[...]
    oh[...] = sh[:, :CLASSES_HALF]
    block = pltpu.roll(osum[:, pl.ds(aligned(owner // N4 * BAND, BAND), BAND)], BAND - 32 * lax.rem(owner, N4), N1)
    for ref, (name, num) in zip(vec_out, VECTORS):
        at = ROW_VEC[name]
        ref[...] = block[at:at + num, :32]
    deep = osum[:, pl.ds(aligned(lax.rem(owner, N4) * BAND, BAND), BAND)]
    index = lax.broadcasted_iota(jnp.int32, (VEC_ROWS, N1), N0)
    head_row = osum[pl.ds(ROW_VEC['b_head'] + tp, N1), :]
    o_bh[...] = head_row[:, :CLASSES_HALF]
    at = ROW_VEC['loss']
    loss[...] = osum[at:at + N1, :N1]
    for layer in range(N2):
        o2[layer] = s2[layer].T
        chosen = index == ROW_VEC['b_ch1'] + N4 * layer + owner // N4
        o_b1[layer:layer + N1, :] = row_sum(jnp.where(chosen, deep, 0.0))
        found = otok[layer, pl.ds(aligned(fsdp * 32, 32), 32), :]
        o_t1[layer] = found[:, :TOK]
        o_t2[layer] = pltpu.roll(found, 64, N1)[:, :TOK]
        o_bt[layer:layer + N1, :] = found.T[BAND - N8:BAND - N7, :]


def finish_all(*operands):
    vmem = pl.BlockSpec(memory_space=pltpu.VMEM)
    shapes = [(N1, N1), (384, 256), (N2, 64, 1024), (N2, BAND, WIDE), (64, CLASSES_HALF)]
    shapes += [(num, 32) for _, num in VECTORS]
    shapes += [(N2, BAND), (N2, 32), (N1, CLASSES_HALF), (N2, 32, TOK), (N2, 32, TOK)]
    return pl.pallas_call(finish_kernel, out_shape=[jax.ShapeDtypeStruct(shape, F32) for shape in shapes],
                          in_specs=[vmem] * len(operands), out_specs=[vmem] * len(shapes), name='finish')(*operands)


def weight_specs():
    vec_spec = P(CHANNEL_AXES)
    layer_vec = P(None, CHANNEL_AXES)
    return (P('fsdp', 'tp'), vec_spec, layer_vec, layer_vec, P(None, None, 'fsdp'), P(None, 'fsdp'),
            P(None, 'fsdp', None), layer_vec, layer_vec, P(None, 'fsdp', 'tp'), layer_vec,
            P(None, CHANNEL_AXES, None), layer_vec, vec_spec, vec_spec, P('fsdp', 'tp'), P('tp'))


def solution(mesh):
    def step(patches, labels, w_stem, b_stem, ln1_g, ln1_b, w_tok1, b_tok1, w_tok2,
             ln2_g, ln2_b, w_ch1, b_ch1, w_ch2, b_ch2, lnf_g, lnf_b, w_head, b_head):
        def flat(values):
            return values.reshape(N1, -N1)
        by_token = patches.swapaxes(N0, N1)
        w1, w2, xa, xb, t1t, t1, t2, bt, vec, gh, hs, d0 = forward_all(
            by_token, flat(labels), w_stem, w_ch1, w_ch2, w_head, flat(b_stem), ln1_g, ln1_b, ln2_g, ln2_b,
            b_ch2, flat(lnf_g), flat(lnf_b), b_ch1, b_tok1, flat(b_head), w_tok1.swapaxes(N1, N2), w_tok2)
        sums = backward_all(w1, w2, t1t, t1, t2, bt, vec, xa, xb, d0, by_token, gh, hs)
        (loss, g_stem, g_ch1, g_ch2, g_head, gb_stem, g1_g, g1_b, g2_g, g2_b, gb_ch2, gf_g, gf_b,
         gb_ch1, gb_tok1, gb_head, g_tok1, g_tok2) = finish_all(*sums)
        return (loss.reshape(()), g_stem, gb_stem.reshape(-N1), g1_g, g1_b, g_tok1.swapaxes(N1, N2), gb_tok1, g_tok2,
                g2_g, g2_b, g_ch1, gb_ch1, g_ch2, gb_ch2, gf_g.reshape(-N1), gf_b.reshape(-N1), g_head,
                gb_head.reshape(-N1))

    specs = weight_specs()
    return jax.shard_map(step, mesh=mesh, in_specs=(P('fsdp', None, None), P('fsdp')) + specs,
                         out_specs=(P(),) + specs, check_vma=False)
```
